128 devices in a mesh: data: 1, cols: 16 (over z, y), model: 8 (over x, core).
Axes of the slice: x: 4, y: 4, z: 4, core: 2. Of those that a mesh axis runs over, the one named last changes fastest.
Arguments:
- x_in: bfloat16 [8, 128, 128, 128], P('data', None, None, ('model', 'cols'))
- w_conv1: bfloat16 [3, 3, 128, 256], P(None, None, ('model', 'cols'))
- b_conv1: float32 [256], replicated
- w_conv2: bfloat16 [3, 3, 256, 256], replicated
- b_conv2: float32 [256], replicated
Outputs:
- output: float32 [8, 128, 128, 256], P('data', 'model', 'cols')
All inputs are finite; a program needn't handle non-finite values.
Results may differ from the reference program's by a relative error of at most 0.001.
Values are sent between devices in bfloat16 or wider.
A program may use at most 1 GiB of HBM per device.

```python
import jax
import jax.numpy as jnp
from jax import lax

IMAGES = 8
HEIGHT = 128
WIDTH = 128
IN_CHANS = 128
MID_CHANS = 256
OUT_CHANS = 256

CONV_DIMS = ("NHWC", "HWIO", "NHWC")


def setup_inputs(seed: int = 0, part: int = 0) -> dict:
    base_key = jax.random.key(seed)
    part_key = jax.random.fold_in(base_key, part)
    key_w1, key_b1, key_w2, key_b2 = jax.random.split(jax.random.fold_in(base_key, 1000), 4)
    x_in = jax.random.normal(part_key, (IMAGES, HEIGHT, WIDTH, IN_CHANS), jnp.float32)
    w_conv1 = jax.random.normal(key_w1, (3, 3, IN_CHANS, MID_CHANS), jnp.float32) * (9 * IN_CHANS) ** -0.5
    b_conv1 = 0.5 * jax.random.normal(key_b1, (MID_CHANS,), jnp.float32)
    w_conv2 = jax.random.normal(key_w2, (3, 3, MID_CHANS, OUT_CHANS), jnp.float32) * (4.5 * MID_CHANS) ** -0.5
    b_conv2 = 0.5 * jax.random.normal(key_b2, (OUT_CHANS,), jnp.float32)
    return {"x_in": x_in.astype(jnp.bfloat16), "w_conv1": w_conv1.astype(jnp.bfloat16), "b_conv1": b_conv1, "w_conv2": w_conv2.astype(jnp.bfloat16), "b_conv2": b_conv2}


def reference(x_in, w_conv1, b_conv1, w_conv2, b_conv2):
    kernel_one = w_conv1.astype(jnp.float32)
    kernel_two = w_conv2.astype(jnp.float32)

    def one_image(image):
        z_sum = lax.conv_general_dilated(image[None].astype(jnp.float32), kernel_one, (1, 1), "SAME", dimension_numbers=CONV_DIMS)
        act_map = jnp.maximum(z_sum + b_conv1, 0.0).astype(jnp.bfloat16)
        out_map = lax.conv_general_dilated(act_map.astype(jnp.float32), kernel_two, (1, 1), "SAME", dimension_numbers=CONV_DIMS)
        return out_map[0] + b_conv2

    return lax.map(one_image, x_in)
```

```python
import functools

import jax
import jax.numpy as jnp
from jax import lax
from jax.experimental import pallas as pl
from jax.experimental.pallas import tpu as pltpu
from jax.sharding import PartitionSpec as P

MESH = pl.DeviceIdType.MESH
GROUP_AXES = ("model", "cols")

N_DEV = 128
N_COLS = 16
HALVES = 2
W_ROWS = 10
PIX = 80
WIN = 12 * PIX
MID = 10 * PIX
C1 = 128
C2 = 256


def dot(a, b):
    return lax.dot_general(a, b, (((1,), (0,)), ((), ())), preferred_element_type=jnp.float32)


def dot_t(a, b):
    return lax.dot_general(a, b, (((0,), (0,)), ((), ())), preferred_element_type=jnp.float32)


def kernel(x_hbm, w1_ref, b1_ref, w2_hbm, b2_ref, out_ref,
           x_loc, pick, sel, place, s_w, s_x0, s_x1, r_w, r_w2, r_x0, r_x1,
           w1_mat, w2_mat, tmp, wtmp, xt, xs, mid, ys, inside, res,
           sem_x, sem_w2, send_w, send_x0, send_x1, send_d, recv_w, recv_x0, recv_x1, recv_d):
    m = lax.axis_index("model")
    c = lax.axis_index("cols")
    me = m * N_COLS + c
    core = m % 2

    def peer_of(step):
        dz = (2 + step // 32) % 4
        dy = (2 + (step // 8) % 4) % 4
        dx = (2 + (step // 2) % 4) % 4
        dk = 1 - step % 2
        px = (m // 2 + dx) % 4
        pk = (core + dk) % 2
        pz = (c // 4 + dz) % 4
        py = (c % 4 + dy) % 4
        return px * 2 + pk, pz * 4 + py

    SELF = 2 * 32 + 2 * 8 + 2 * 2 + 1

    def each_peer(body):
        def step(i, carry):
            body(*peer_of(i))
            return carry
        lax.fori_loop(0, SELF, step, 0)
        lax.fori_loop(SELF + 1, N_DEV, step, 0)

    barrier = pltpu.get_barrier_semaphore()

    def greet(pm, pc):
        pl.semaphore_signal(barrier, inc=1, device_id={"model": pm, "cols": pc}, device_id_type=MESH)

    each_peer(greet)
    get_x = pltpu.make_async_copy(x_hbm, x_loc, sem_x)
    get_x.start()
    get_w2 = pltpu.make_async_copy(w2_hbm, w2_mat, sem_w2)
    get_w2.start()

    for k in range(2):
        for j in range(4):
            tap = j + 5 * k
            for half in range(2):
                s_w[k, 2 * j + half : 2 * j + half + 1, :] = w1_ref[tap // 3, tap % 3 : tap % 3 + 1, half * 128 : half * 128 + 128]
        s_w[k, 8:9, :] = w1_ref[1, 1:2, k * 128 : k * 128 + 128]
        s_w[k, 9:10, :] = jnp.zeros((1, 128), jnp.bfloat16)

    for blk in range(4):
        lane = blk * 512 + lax.broadcasted_iota(jnp.int32, (1, 512), 1)
        img = lane % 4
        if blk < 2:
            row = (lane // 128) * 16 + (lane // 4) % 16
            at = img * 128 + row
        else:
            h = (lane // 4) % 4
            row = (lane // 128 - 8) * 16 + h - 2 + jnp.where(h >= 2, 16, 0)
            at = jnp.where((row >= 0) & (row < 128), img * 128 + row, -1)
        rows = lax.broadcasted_iota(jnp.int32, (512, 512), 0)
        pick[:, blk * 512 : blk * 512 + 512] = jnp.where(rows == at, 1.0, 0.0).astype(jnp.bfloat16)
    r_id = lax.broadcasted_iota(jnp.int32, (128, 256), 0)
    k_id = lax.broadcasted_iota(jnp.int32, (128, 256), 1)
    first = (r_id // 8) * 8 - 2
    s_id = r_id % 8
    main = (s_id < 6) & ((k_id == first + 2 * s_id) | (k_id == first + 2 * s_id + 1)) & (k_id < 128)
    edge0 = (s_id == 6) & (k_id >= 128 + jnp.maximum(first, 0)) & (k_id < 128 + first + 8)
    edge1 = (s_id == 7) & (k_id >= 128 + first + 8) & (k_id < 128 + first + 12)
    place[...] = jnp.where(main | edge0 | edge1, 1.0, 0.0).astype(jnp.bfloat16)
    p_id = lax.broadcasted_iota(jnp.int32, (MID, 128), 0)
    at_row = m * 16 - 1 + (p_id % PIX) // 4
    at_col = c * 8 - 1 + p_id // PIX
    inside[...] = jnp.where((at_row >= 0) & (at_row < 128) & (at_col >= 0) & (at_col < 128), 1.0, 0.0)

    get_x.wait()
    w_id = lax.broadcasted_iota(jnp.int32, (128, 512), 0)
    l_id = lax.broadcasted_iota(jnp.int32, (128, 512), 1) % 128
    keep_main = (l_id // 64) == (w_id % 2)
    keep_edge = (l_id // 16) == ((w_id + 2) % 8)
    for q, s_x in enumerate((s_x0, s_x1)):
        img = x_loc[4 * q : 4 * q + 4].reshape(512, 128)
        for blk in range(4):
            z = dot_t(img, pick[:, blk * 512 : blk * 512 + 512])
            keep = keep_main if blk < 2 else keep_edge
            top = 0 if blk < 2 else 128
            sel[top : top + 128, (blk % 2) * 512 : (blk % 2) * 512 + 512] = jnp.where(keep, z, 0.0).astype(jnp.bfloat16)
        for blk in range(2):
            t = dot(place[...], sel[:, blk * 512 : blk * 512 + 512]).astype(jnp.bfloat16)
            for r in range(4):
                tiles = t[:, r * 128 : r * 128 + 128].reshape(16, 8, 128)
                s_x[(blk * 4 + r) * 16 : (blk * 4 + r) * 16 + 16] = tiles

    pl.semaphore_wait(barrier, N_DEV - 1)

    def send(src, dst, send_sem, recv_sem, pm, pc):
        pltpu.make_async_remote_copy(src_ref=src, dst_ref=dst, send_sem=send_sem, recv_sem=recv_sem,
                                     device_id={"model": pm, "cols": pc}, device_id_type=MESH).start()

    each_peer(lambda pm, pc: send(s_w.at[pm % 2], r_w.at[me], send_w, recv_w, pm, pc))
    each_peer(lambda pm, pc: send(s_x0.at[pm * N_COLS + pc], r_x0.at[me], send_x0, recv_x0, pm, pc))
    each_peer(lambda pm, pc: send(s_x1.at[pm * N_COLS + pc], r_x1.at[me], send_x1, recv_x1, pm, pc))
    r_w[pl.ds(me, 1)] = s_w[pl.ds(core, 1)]
    r_x0[pl.ds(me, 1)] = s_x0[pl.ds(me, 1)]
    r_x1[pl.ds(me, 1)] = s_x1[pl.ds(me, 1)]

    def drain(ref, sem):
        part = ref.at[pl.ds(0, N_DEV - 1)]
        pltpu.make_async_copy(part, part, sem).wait()

    def unpack_w(ref, k):
        wtmp[...] = ref[...].astype(jnp.float32).reshape(N_DEV * W_ROWS, 128)
        for s in range(9):
            rows = wtmp[pl.ds(s, N_DEV, stride=W_ROWS), :].astype(jnp.bfloat16)
            if s == 8:
                w1_mat[pl.ds(4 * C1, C1), pl.ds(pl.multiple_of(k * 128, 128), 128)] = rows
            else:
                tap = 5 * k + s // 2
                w1_mat[pl.ds(pl.multiple_of(tap * C1, C1), C1), (s % 2) * 128 : (s % 2) * 128 + 128] = rows

    drain(r_w, recv_w)
    swap = pltpu.make_async_remote_copy(src_ref=r_w, dst_ref=r_w2, send_sem=send_d, recv_sem=recv_d,
                                        device_id={"model": m + 1 - 2 * core, "cols": c}, device_id_type=MESH)
    swap.start()
    unpack_w(r_w, core)
    swap.wait_recv()
    unpack_w(r_w2, 1 - core)
    get_w2.wait()

    for q, (r_x, recv_x) in enumerate(((r_x0, recv_x0), (r_x1, recv_x1))):
        drain(r_x, recv_x)
        tmp[...] = r_x[...].astype(jnp.float32).reshape(N_DEV * 8, 128)
        for s in range(8):
            t = tmp[pl.ds(s, N_DEV, stride=8), :].T
            if s < 6:
                for par in range(2):
                    at = (2 * s + par) * PIX + 8
                    xt[at : at + 64, :] = t[par * 64 : par * 64 + 64]
            else:
                for j in range(8 if s == 6 else 4):
                    at = ((s - 6) * 8 + j) * PIX
                    xt[at : at + 8, :] = t[16 * j : 16 * j + 8]
                    xt[at + 72 : at + 80, :] = t[16 * j + 8 : 16 * j + 16]
        for dh in range(3):
            n = WIN - (0 if dh == 0 else 16)
            xs[dh, 0:n, :] = xt[4 * dh : 4 * dh + n, :].astype(jnp.bfloat16)
            if dh:
                xs[dh, n:WIN, :] = jnp.zeros((16, C1), jnp.bfloat16)
                xs[dh, n : n + 8, :] = xt[n + 4 * dh : n + 4 * dh + 8, :].astype(jnp.bfloat16)
        half_m = MID // 2
        for mc in range(2):
            acc = None
            for pair in range(5):
                lhs = []
                for tap in range(2 * pair, min(2 * pair + 2, 9)):
                    dh, dw = tap // 3, tap % 3
                    lhs.append(xs[dh, dw * PIX + mc * half_m : dw * PIX + mc * half_m + half_m, :])
                lhs = jnp.concatenate(lhs, axis=1) if len(lhs) > 1 else lhs[0]
                part = dot(lhs, w1_mat[pair * 256 : pair * 256 + lhs.shape[1], :])
                acc = part if acc is None else acc + part
            act = jnp.maximum(acc + b1_ref[...], 0.0)
            ok = inside[mc * half_m : mc * half_m + half_m, :] > 0.0
            mid[mc * half_m : mc * half_m + half_m, 0:128] = jnp.where(ok, act[:, 0:128], 0.0)
            mid[mc * half_m : mc * half_m + half_m, 128:256] = jnp.where(ok, act[:, 128:256], 0.0)
        for dh in range(3):
            for wc in range(10):
                ys[dh, wc] = mid[wc * PIX + 4 * dh : wc * PIX + 4 * dh + 64, :].astype(jnp.bfloat16)
        acc = None
        for tap in range(9):
            dh, dw = tap // 3, tap % 3
            part = dot(ys[dh, dw : dw + 8].reshape(512, C2), w2_mat[dh, dw])
            acc = part if acc is None else acc + part
        full = acc + b2_ref[...]
        res[0] = full[:, 0:128]
        res[1] = full[:, 128:256]
        for h in range(16):
            for n in range(4):
                for half in range(2):
                    cols = slice(half * 128, half * 128 + 128)
                    out_ref[4 * q + n, h, :, cols] = res.at[half][pl.ds(h * 4 + n, 8, stride=64), :]

    def drain_send(ref, sem):
        part = ref.at[pl.ds(0, N_DEV - 1)]
        pltpu.make_async_copy(part, part, sem).wait()

    drain_send(r_w, send_w)
    drain_send(s_x0, send_x0)
    drain_send(s_x1, send_x1)
    swap.wait_send()


def solution(mesh):
    def run_local(x_in, w_conv1, b_conv1, w_conv2, b_conv2):
        bf, f32 = jnp.bfloat16, jnp.float32
        vmem = pl.BlockSpec(memory_space=pltpu.VMEM)
        hbm = pl.BlockSpec(memory_space=pl.ANY)
        dma = pltpu.SemaphoreType.DMA
        x = x_in.reshape(x_in.shape[:3])
        w1 = w_conv1.reshape(3, 3, 256)
        return pl.pallas_call(
            kernel,
            name="conv_pair",
            out_shape=jax.ShapeDtypeStruct((8, 16, 8, C2), f32),
            in_specs=[hbm, vmem, vmem, hbm, vmem],
            out_specs=vmem,
            scratch_shapes=[
                pltpu.VMEM((8, 128, 128), bf),
                pltpu.VMEM((512, 2048), bf),
                pltpu.VMEM((256, 1024), bf),
                pltpu.VMEM((128, 256), bf),
                pltpu.VMEM((2, W_ROWS, 128), bf),
                pltpu.VMEM((N_DEV, 8, 128), bf),
                pltpu.VMEM((N_DEV, 8, 128), bf),
                pltpu.VMEM((N_DEV, W_ROWS, 128), bf),
                pltpu.VMEM((N_DEV, W_ROWS, 128), bf),
                pltpu.VMEM((N_DEV, 8, 128), bf),
                pltpu.VMEM((N_DEV, 8, 128), bf),
                pltpu.VMEM((9 * C1, C2), bf),
                pltpu.VMEM((3, 3, C2, C2), bf),
                pltpu.VMEM((N_DEV * 8, 128), f32),
                pltpu.VMEM((N_DEV * W_ROWS, 128), f32),
                pltpu.VMEM((WIN, C1), f32),
                pltpu.VMEM((3, WIN, C1), bf),
                pltpu.VMEM((MID, C2), f32),
                pltpu.VMEM((3, 10, 64, C2), bf),
                pltpu.VMEM((MID, 128), f32),
                pltpu.VMEM((2, 512, 128), f32),
            ] + [dma] * 10,
            compiler_params=pltpu.CompilerParams(collective_id=0, has_side_effects=True, vmem_limit_bytes=60 << 20),
        )(x, w1, b_conv1.reshape(1, 256), w_conv2, b_conv2.reshape(1, 256))

    return jax.shard_map(
        run_local,
        mesh=mesh,
        in_specs=(P("data", None, None, GROUP_AXES), P(None, None, GROUP_AXES, None), P(), P(), P()),
        out_specs=P("data", "model", "cols", None),
        check_vma=False,
    )
```

```python
import functools

import jax
import jax.numpy as jnp
from jax import lax
from jax.experimental import pallas as pl
from jax.experimental.pallas import tpu as pltpu
from jax.sharding import PartitionSpec as P

MESH = pl.DeviceIdType.MESH
GROUP_AXES = ("model", "cols")

N_DEV = 128
N_COLS = 16
HALVES = 2
PIX = 80
WIN = 12 * PIX
MID = 10 * PIX
C1 = 128
C2 = 256


def dot(a, b):
    return lax.dot_general(a, b, (((1,), (0,)), ((), ())), preferred_element_type=jnp.float32)


def dot_t(a, b):
    return lax.dot_general(a, b, (((0,), (0,)), ((), ())), preferred_element_type=jnp.float32)


def kernel(x_hbm, w1_hbm, b1_hbm, w2_hbm, b2_hbm, out_ref, ys, w2_mat,
           x_loc, w1_loc, b1_loc, b2_loc, pick, sel, place, s_w, s_t, s_x0, s_x1, r_w, r_w2, r_t, r_x0, r_x1,
           w1_mat, tmp, xt, xs, mid, inside, res,
           sem_x, sem_w1, sem_b, sem_w2, send_w, send_t, send_x0, send_x1, send_d,
           recv_w, recv_t, recv_x0, recv_x1, recv_d):
    m = lax.axis_index("model")
    c = lax.axis_index("cols")
    me = m * N_COLS + c
    core = m % 2

    get_x = pltpu.make_async_copy(x_hbm, x_loc, sem_x)
    get_x.start()
    get_w1 = pltpu.make_async_copy(w1_hbm, w1_loc, sem_w1)
    get_w1.start()
    get_b = (pltpu.make_async_copy(b1_hbm, b1_loc, sem_b.at[0]), pltpu.make_async_copy(b2_hbm, b2_loc, sem_b.at[1]))
    for get in get_b:
        get.start()
    get_w2 = pltpu.make_async_copy(w2_hbm, w2_mat, sem_w2)
    get_w2.start()

    pms = [((m // 2 + dx) % 4) * 2 + (core + dk) % 2 for dx in (2, 1, 3, 0) for dk in (1, 0)]

    def each_peer(body):
        def step(i, carry):
            tz, ty = i // 4, i % 4
            dz = (2 + tz) % 4 + (tz // 2) * (1 - 2 * (tz % 2))
            dy = (2 + ty) % 4 + (ty // 2) * (1 - 2 * (ty % 2))
            pc = ((c // 4 + dz) % 4) * 4 + (c % 4 + dy) % 4
            for pm in pms:
                body(pm, pc)
            return carry
        lax.fori_loop(0, 15, step, 0)
        for pm in pms[:-1]:
            body(pm, c)

    barrier = pltpu.get_barrier_semaphore()

    def greet(pm, pc):
        pl.semaphore_signal(barrier, inc=1, device_id={"model": pm, "cols": pc}, device_id_type=MESH)

    each_peer(greet)

    for blk in range(4):
        lane = blk * 512 + lax.broadcasted_iota(jnp.int32, (1, 512), 1)
        img = lane % 4
        if blk < 2:
            row = (lane // 128) * 16 + (lane // 4) % 16
            at = img * 128 + row
        else:
            h = (lane // 4) % 4
            row = (lane // 128 - 8) * 16 + h - 2 + jnp.where(h >= 2, 16, 0)
            at = jnp.where((row >= 0) & (row < 128), img * 128 + row, -1)
        rows = lax.broadcasted_iota(jnp.int32, (512, 512), 0)
        pick[:, blk * 512 : blk * 512 + 512] = jnp.where(rows == at, 1.0, 0.0).astype(jnp.bfloat16)
    r_id = lax.broadcasted_iota(jnp.int32, (128, 256), 0)
    k_id = lax.broadcasted_iota(jnp.int32, (128, 256), 1)
    first = (r_id // 8) * 8 - 2
    s_id = r_id % 8
    main = (s_id < 6) & ((k_id == first + 2 * s_id) | (k_id == first + 2 * s_id + 1)) & (k_id < 128)
    edge0 = (s_id == 6) & (k_id >= 128 + jnp.maximum(first, 0)) & (k_id < 128 + first + 8)
    edge1 = (s_id == 7) & (k_id >= 128 + first + 8) & (k_id < 128 + first + 12)
    place[...] = jnp.where(main | edge0 | edge1, 1.0, 0.0).astype(jnp.bfloat16)
    p_id = lax.broadcasted_iota(jnp.int32, (MID, 128), 0)
    at_row = m * 16 - 1 + (p_id % PIX) // 4
    at_col = c * 8 - 1 + p_id // PIX
    inside[...] = jnp.where((at_row >= 0) & (at_row < 128) & (at_col >= 0) & (at_col < 128), 1.0, 0.0)

    get_w1.wait()
    for tap in range(9):
        for half in range(2):
            row = w1_loc[tap // 3, tap % 3 : tap % 3 + 1, half * 128 : half * 128 + 128]
            if tap < 8:
                at = 2 * (tap % 4) + half
                s_w[tap // 4, at : at + 1, :] = row
            else:
                s_t[half : half + 1, :] = row

    pl.semaphore_wait(barrier, N_DEV - 1)

    def send(src, dst, send_sem, recv_sem, pm, pc):
        pltpu.make_async_remote_copy(src_ref=src, dst_ref=dst, send_sem=send_sem, recv_sem=recv_sem,
                                     device_id={"model": pm, "cols": pc}, device_id_type=MESH).start()

    def send_weights(pm, pc):
        send(s_w.at[pm % 2], r_w.at[me], send_w, recv_w, pm, pc)
        send(s_t, r_t.at[me], send_t, recv_t, pm, pc)

    each_peer(send_weights)

    get_x.wait()
    w_id = lax.broadcasted_iota(jnp.int32, (128, 512), 0)
    l_id = lax.broadcasted_iota(jnp.int32, (128, 512), 1) % 128
    keep_main = (l_id // 64) == (w_id % 2)
    keep_edge = (l_id // 16) == ((w_id + 2) % 8)
    for q, s_x in enumerate((s_x0, s_x1)):
        img = x_loc[4 * q : 4 * q + 4].reshape(512, 128)
        for blk in range(4):
            z = dot_t(img, pick[:, blk * 512 : blk * 512 + 512])
            keep = keep_main if blk < 2 else keep_edge
            top = 0 if blk < 2 else 128
            sel[top : top + 128, (blk % 2) * 512 : (blk % 2) * 512 + 512] = jnp.where(keep, z, 0.0).astype(jnp.bfloat16)
        for blk in range(2):
            t = dot(place[...], sel[:, blk * 512 : blk * 512 + 512]).astype(jnp.bfloat16)
            for r in range(4):
                tiles = t[:, r * 128 : r * 128 + 128].reshape(16, 8, 128)
                s_x[(blk * 4 + r) * 16 : (blk * 4 + r) * 16 + 16] = tiles

    each_peer(lambda pm, pc: send(s_x0.at[pm * N_COLS + pc], r_x0.at[me], send_x0, recv_x0, pm, pc))
    each_peer(lambda pm, pc: send(s_x1.at[pm * N_COLS + pc], r_x1.at[me], send_x1, recv_x1, pm, pc))
    r_w[pl.ds(me, 1)] = s_w[pl.ds(core, 1)]
    r_t[pl.ds(me, 1)] = s_t[...].reshape(1, 2, 128)
    r_x0[pl.ds(me, 1)] = s_x0[pl.ds(me, 1)]
    r_x1[pl.ds(me, 1)] = s_x1[pl.ds(me, 1)]

    def drain(ref, sem):
        part = ref.at[pl.ds(0, N_DEV - 1)]
        pltpu.make_async_copy(part, part, sem).wait()

    def unpack_w(ref, k):
        tmp[...] = ref[...].astype(jnp.float32).reshape(N_DEV * 8, 128)
        for s in range(8):
            rows = tmp[pl.ds(s, N_DEV, stride=8), :].astype(jnp.bfloat16)
            at = pl.multiple_of((4 * k + s // 2) * C1, C1)
            w1_mat[pl.ds(at, C1), (s % 2) * 128 : (s % 2) * 128 + 128] = rows

    drain(r_w, recv_w)
    swap = pltpu.make_async_remote_copy(src_ref=r_w, dst_ref=r_w2, send_sem=send_d, recv_sem=recv_d,
                                        device_id={"model": m + 1 - 2 * core, "cols": c}, device_id_type=MESH)
    swap.start()
    unpack_w(r_w, core)
    drain(r_t, recv_t)
    tmp[0 : 2 * N_DEV] = r_t[...].astype(jnp.float32).reshape(N_DEV * 2, 128)
    for half in range(2):
        w1_mat[8 * C1 : 9 * C1, half * 128 : half * 128 + 128] = tmp[pl.ds(half, N_DEV, stride=2), :].astype(jnp.bfloat16)
    swap.wait_recv()
    unpack_w(r_w2, 1 - core)
    for get in get_b:
        get.wait()
    get_w2.wait()

    for q, (r_x, recv_x) in enumerate(((r_x0, recv_x0), (r_x1, recv_x1))):
        drain(r_x, recv_x)
        tmp[...] = r_x[...].astype(jnp.float32).reshape(N_DEV * 8, 128)
        for s in range(8):
            t = tmp[pl.ds(s, N_DEV, stride=8), :].T
            if s < 6:
                for par in range(2):
                    at = (2 * s + par) * PIX + 8
                    xt[at : at + 64, :] = t[par * 64 : par * 64 + 64]
            else:
                for j in range(8 if s == 6 else 4):
                    at = ((s - 6) * 8 + j) * PIX
                    xt[at : at + 8, :] = t[16 * j : 16 * j + 8]
                    xt[at + 72 : at + 80, :] = t[16 * j + 8 : 16 * j + 16]
        for dh in range(3):
            n = WIN - (0 if dh == 0 else 16)
            xs[dh, 0:n, :] = xt[4 * dh : 4 * dh + n, :].astype(jnp.bfloat16)
            if dh:
                xs[dh, n:WIN, :] = jnp.zeros((16, C1), jnp.bfloat16)
                xs[dh, n : n + 8, :] = xt[n + 4 * dh : n + 4 * dh + 8, :].astype(jnp.bfloat16)
        half_m = MID // 2
        for mc in range(2):
            acc = None
            for pair in range(5):
                lhs = []
                for tap in range(2 * pair, min(2 * pair + 2, 9)):
                    dh, dw = tap // 3, tap % 3
                    lhs.append(xs[dh, dw * PIX + mc * half_m : dw * PIX + mc * half_m + half_m, :])
                lhs = jnp.concatenate(lhs, axis=1) if len(lhs) > 1 else lhs[0]
                part = dot(lhs, w1_mat[pair * 256 : pair * 256 + lhs.shape[1], :])
                acc = part if acc is None else acc + part
            act = jnp.maximum(acc + b1_loc[...], 0.0)
            ok = inside[mc * half_m : mc * half_m + half_m, :] > 0.0
            mid[mc * half_m : mc * half_m + half_m, 0:128] = jnp.where(ok, act[:, 0:128], 0.0)
            mid[mc * half_m : mc * half_m + half_m, 128:256] = jnp.where(ok, act[:, 128:256], 0.0)
        for dh in range(3):
            for wc in range(10):
                ys[dh, wc] = mid[wc * PIX + 4 * dh : wc * PIX + 4 * dh + 64, :].astype(jnp.bfloat16)
        if q == 0:
            conv_two(ys, w2_mat, b2_loc, res)
            unscramble(res, out_ref)

    def drain_send(ref, sem):
        part = ref.at[pl.ds(0, N_DEV - 1)]
        pltpu.make_async_copy(part, part, sem).wait()

    drain_send(r_w, send_w)
    drain_send(r_t, send_t)
    drain_send(s_x0, send_x0)
    drain_send(s_x1, send_x1)
    swap.wait_send()


def conv_two(ys, w2_mat, b2_ref, res):
    acc = None
    for tap in range(9):
        dh, dw = tap // 3, tap % 3
        part = dot(ys[dh, dw : dw + 8].reshape(512, C2), w2_mat[dh, dw])
        acc = part if acc is None else acc + part
    full = acc + b2_ref[...]
    res[0] = full[:, 0:128]
    res[1] = full[:, 128:256]


def unscramble(res, out_ref):
    for n in range(4):
        for h in range(16):
            for half in range(2):
                out_ref[n, h, :, half * 128 : half * 128 + 128] = res.at[half][pl.ds(h * 4 + n, 8, stride=64), :]


def kernel_two(out0, ys, w2_mat, b2_ref, out_hbm, out1, res, sem):
    put0 = pltpu.make_async_copy(out0, out_hbm.at[0:4], sem.at[0])
    put0.start()
    conv_two(ys, w2_mat, b2_ref, res)
    unscramble(res, out1)
    put1 = pltpu.make_async_copy(out1, out_hbm.at[4:8], sem.at[1])
    put1.start()
    put0.wait()
    put1.wait()


def solution(mesh):
    def run_local(x_in, w_conv1, b_conv1, w_conv2, b_conv2):
        bf, f32 = jnp.bfloat16, jnp.float32
        vmem = pl.BlockSpec(memory_space=pltpu.VMEM)
        hbm = pl.BlockSpec(memory_space=pltpu.HBM)
        dma = pltpu.SemaphoreType.DMA
        x = x_in.reshape(x_in.shape[:3])
        w1 = w_conv1.reshape(3, 3, 256)
        b2 = b_conv2.reshape(1, 256)
        out0, ys, w2 = pl.pallas_call(
            kernel,
            name="conv_pair",
            out_shape=[
                jax.ShapeDtypeStruct((4, 16, 8, C2), f32),
                jax.ShapeDtypeStruct((3, 10, 64, C2), bf),
                jax.ShapeDtypeStruct((3, 3, C2, C2), bf),
            ],
            in_specs=[hbm] * 5,
            out_specs=[vmem] * 3,
            scratch_shapes=[
                pltpu.VMEM((8, 128, 128), bf),
                pltpu.VMEM((3, 3, C2), bf),
                pltpu.VMEM((1, C2), f32),
                pltpu.VMEM((1, C2), f32),
                pltpu.VMEM((512, 2048), bf),
                pltpu.VMEM((256, 1024), bf),
                pltpu.VMEM((128, 256), bf),
                pltpu.VMEM((2, 8, 128), bf),
                pltpu.VMEM((2, 128), bf),
                pltpu.VMEM((N_DEV, 8, 128), bf),
                pltpu.VMEM((N_DEV, 8, 128), bf),
                pltpu.VMEM((N_DEV, 8, 128), bf),
                pltpu.VMEM((N_DEV, 8, 128), bf),
                pltpu.VMEM((N_DEV, 2, 128), bf),
                pltpu.VMEM((N_DEV, 8, 128), bf),
                pltpu.VMEM((N_DEV, 8, 128), bf),
                pltpu.VMEM((9 * C1, C2), bf),
                pltpu.VMEM((N_DEV * 8, 128), f32),
                pltpu.VMEM((WIN, C1), f32),
                pltpu.VMEM((3, WIN, C1), bf),
                pltpu.VMEM((MID, C2), f32),
                pltpu.VMEM((MID, 128), f32),
                pltpu.VMEM((2, 512, 128), f32),
                dma, dma, pltpu.SemaphoreType.DMA((2,)),
            ] + [dma] * 11,
            compiler_params=pltpu.CompilerParams(collective_id=0, has_side_effects=True, vmem_limit_bytes=24 << 20),
        )(*(pltpu.with_memory_space_constraint(a, pltpu.HBM) for a in (x, w1, b_conv1.reshape(1, 256), w_conv2, b2)))
        return pl.pallas_call(
            kernel_two,
            name="conv_last",
            out_shape=jax.ShapeDtypeStruct((8, 16, 8, C2), f32),
            in_specs=[vmem] * 4,
            out_specs=hbm,
            scratch_shapes=[pltpu.VMEM((4, 16, 8, C2), f32), pltpu.VMEM((2, 512, 128), f32), pltpu.SemaphoreType.DMA((2,))],
            compiler_params=pltpu.CompilerParams(vmem_limit_bytes=24 << 20),
        )(out0, ys, w2, b2)

    return jax.shard_map(
        run_local,
        mesh=mesh,
        in_specs=(P("data", None, None, GROUP_AXES), P(None, None, GROUP_AXES, None), P(), P(), P()),
        out_specs=P("data", "model", "cols", None),
        check_vma=False,
    )
```

```python
import collections
import functools

import jax
import jax.numpy as jnp
from jax import lax
from jax.experimental import pallas as pl
from jax.experimental.pallas import tpu as pltpu
from jax.sharding import PartitionSpec as P

MESH = pl.DeviceIdType.MESH
GROUP_AXES = ("model", "cols")

N_DEV = 128
N_COLS = 16
COL = 160
MID_COL = 144
OUT_COL = 136
C1 = 128
C2 = 256
HOPS = (0, 1, 2, 1)


def peer_order():
    def links(shift):
        used = collections.Counter()
        for axis, d in enumerate(shift[:3]):
            if d in (1, 2):
                used[axis, 0] += 1
            if d in (3, 2):
                used[axis, 1] += 1
        return used

    shifts = [(dx, dy, dz, dk) for dx in range(4) for dy in range(4) for dz in range(4) for dk in range(2)][1:]
    load, order = collections.Counter(), []
    for tail in range(4, -1, -1):
        rest = [s for s in shifts if HOPS[s[1]] + HOPS[s[2]] == tail]
        while rest:
            def cost(s):
                new = load + links(s)
                return max(new.values(), default=0) * 100 + sum(v * v for v in new.values()) * 0.01
            best = min(rest, key=cost)
            rest.remove(best)
            order.append(best)
            load += links(best)
    return order


ORDER = peer_order()


def dot(a, b):
    return lax.dot_general(a, b, (((1,), (0,)), ((), ())), preferred_element_type=jnp.float32)


def kernel(x_hbm, w1_hbm, b1_hbm, w2_hbm, b2_hbm, out_ref,
           x_loc, w1_loc, b1_loc, b2_loc, w2_mat, turned, pick, sel, place, s_w, s_x, r_w, r_w2, r_x,
           w1_mat, tmp, edge, xs0, xs8, ys0, ys8, inside, res,
           sem_x, sem_w1, sem_b, sem_w2, send_w, send_x, send_d, recv_w, recv_x, recv_d):
    m = lax.axis_index("model")
    c = lax.axis_index("cols")
    me = m * N_COLS + c
    core = m % 2

    get_x = pltpu.make_async_copy(x_hbm, x_loc, sem_x)
    get_x.start()
    get_w1 = pltpu.make_async_copy(w1_hbm, w1_loc, sem_w1)
    get_w1.start()
    get_b = (pltpu.make_async_copy(b1_hbm, b1_loc, sem_b.at[0]), pltpu.make_async_copy(b2_hbm, b2_loc, sem_b.at[1]))
    for get in get_b:
        get.start()
    get_w2 = pltpu.make_async_copy(w2_hbm, w2_mat, sem_w2)
    get_w2.start()

    cores = (core, 1 - core)
    models = [[((m // 2 + dx) % 4) * 2 + k for k in cores] for dx in range(4)]
    cols_y = [(c % 4 + dy) % 4 for dy in range(4)]
    cols = [[((c // 4 + dz) % 4) * 4 + y for y in cols_y] for dz in range(4)]

    def each_peer(body):
        for dx, dy, dz, dk in ORDER:
            body(models[dx][dk], cols[dz][dy], cores[dk])

    barrier = pltpu.get_barrier_semaphore()

    def greet(pm, pc, pk):
        pl.semaphore_signal(barrier, inc=1, device_id={"model": pm, "cols": pc}, device_id_type=MESH)

    each_peer(greet)

    for blk in range(4):
        lane = blk * 512 + lax.broadcasted_iota(jnp.int32, (1, 512), 1)
        img = lane % 8
        if blk < 2:
            row = (lane // 128) * 16 + (lane // 8) % 16
        else:
            h = (lane // 8) % 4
            row = (lane // 128 - 8) * 16 + h - 2 + jnp.where(h >= 2, 16, 0)
        at = jnp.where((row >= 0) & (row < 128), img * 128 + row, -1)
        for pair in range(4):
            rows = pair * 256 + lax.broadcasted_iota(jnp.int32, (256, 512), 0)
            pick[pair * 256 : pair * 256 + 256, blk * 512 : blk * 512 + 512] = jnp.where(rows == at, 1.0, 0.0).astype(jnp.bfloat16)
    r_id = lax.broadcasted_iota(jnp.int32, (256, 256), 0)
    k_id = lax.broadcasted_iota(jnp.int32, (256, 256), 1)
    first = (r_id // 16) * 8 - 2
    s_id = r_id % 16
    main = (s_id < 12) & (k_id == first + s_id) & (k_id < 128)
    from_col = first + 4 * (s_id - 12)
    border = (s_id >= 12) & (s_id < 15) & (k_id >= 128 + jnp.maximum(from_col, 0)) & (k_id < 132 + from_col)
    place[...] = jnp.where(main | border, 1.0, 0.0).astype(jnp.bfloat16)
    p_id = lax.broadcasted_iota(jnp.int32, (10 * MID_COL, 128), 0)
    at_row = m * 16 - 1 + (p_id % MID_COL) // 8
    at_col = c * 8 - 1 + p_id // MID_COL
    inside[...] = jnp.where((at_row >= 0) & (at_row < 128) & (at_col >= 0) & (at_col < 128), 1.0, 0.0).reshape(10, MID_COL, 128)

    get_w1.wait()
    for k in range(2):
        for j in range(4):
            tap = 4 * k + j
            s_w[k, j] = jnp.concatenate([w1_loc[tap // 3, tap % 3 : tap % 3 + 1, half * 128 : half * 128 + 128] for half in range(2)])
        last = w1_loc[2, 2:3, k * 128 : k * 128 + 128]
        s_w[k, 4] = jnp.concatenate([last, jnp.zeros_like(last)])

    get_x.wait()
    for n in range(8):
        turned[:, n * 128 : n * 128 + 128] = x_loc[n].T
    w_id = lax.broadcasted_iota(jnp.int32, (128, 256), 0)
    l_id = lax.broadcasted_iota(jnp.int32, (128, 256), 1) % 128
    keep = (l_id // 32) == ((w_id + 2) % 4)
    for blk in range(8):
        z = None
        for pair in range(4):
            term = dot(turned[:, pair * 256 : pair * 256 + 256], pick[pair * 256 : pair * 256 + 256, blk * 256 : blk * 256 + 256])
            z = term if z is None else z + term
        if blk >= 4:
            z = jnp.where(keep, z, 0.0)
        top = 0 if blk < 4 else 128
        sel[top : top + 128, (blk % 4) * 256 : (blk % 4) * 256 + 256] = z.astype(jnp.bfloat16)
    for blk in range(4):
        t = dot(place[...], sel[:, blk * 256 : blk * 256 + 256])
        for r in range(2):
            tiles = t[:, r * 128 : r * 128 + 128].reshape(16, 2, 8, 128).astype(jnp.bfloat16)
            s_x[(blk * 2 + r) * 16 : (blk * 2 + r) * 16 + 16] = tiles

    pl.semaphore_wait(barrier, N_DEV - 1)

    def send(src, dst, send_sem, recv_sem, pm, pc):
        pltpu.make_async_remote_copy(src_ref=src, dst_ref=dst, send_sem=send_sem, recv_sem=recv_sem,
                                     device_id={"model": pm, "cols": pc}, device_id_type=MESH).start()

    each_peer(lambda pm, pc, pk: send(s_w.at[pk], r_w.at[me], send_w, recv_w, pm, pc))
    each_peer(lambda pm, pc, pk: send(s_x.at[pm * N_COLS + pc], r_x.at[me], send_x, recv_x, pm, pc))
    r_w[pl.ds(me, 1)] = s_w[pl.ds(core, 1)]
    r_x[pl.ds(me, 1)] = s_x[pl.ds(me, 1)]

    def drain(ref, sem):
        part = ref.at[pl.ds(0, N_DEV - 1)]
        pltpu.make_async_copy(part, part, sem).wait()

    def unpack_w(ref, k):
        for j in range(5):
            tmp[0, 0 : 2 * N_DEV] = ref[:, j].astype(jnp.float32).reshape(N_DEV * 2, 128)
            for half in range(2 if j < 4 else 1):
                rows = tmp.at[0][pl.ds(half, N_DEV, stride=2), :].astype(jnp.bfloat16)
                if j < 4:
                    at = pl.multiple_of((4 * k + j) * C1, C1)
                    w1_mat[pl.ds(at, C1), half * 128 : half * 128 + 128] = rows
                else:
                    w1_mat[8 * C1 : 9 * C1, pl.ds(pl.multiple_of(k * 128, 128), 128)] = rows

    drain(r_w, recv_w)
    swap = pltpu.make_async_remote_copy(src_ref=r_w, dst_ref=r_w2, send_sem=send_d, recv_sem=recv_d,
                                        device_id={"model": m + 1 - 2 * core, "cols": c}, device_id_type=MESH)
    swap.start()
    unpack_w(r_w, core)
    swap.wait_recv()
    unpack_w(r_w2, 1 - core)
    for get in get_b:
        get.wait()
    get_w2.wait()

    drain(r_x, recv_x)
    for half in range(2):
        tmp[half] = r_x[:, half].astype(jnp.float32).reshape(N_DEV * 8, 128)

    def pixels(s):
        return tmp.at[s // 8][pl.ds(s % 8, N_DEV, stride=8), :].T

    for s in range(12, 15):
        edge[s - 12] = pixels(s)
    for w in range(12):
        top = (w % 4) * 32
        col = jnp.concatenate([edge[w // 4, top : top + 16], pixels(w), edge[w // 4, top + 16 : top + 32]])
        xs0[w] = col.astype(jnp.bfloat16)
        xs8[w] = col[8 : 8 + MID_COL].astype(jnp.bfloat16)

    for lo, hi in ((0, 3), (3, 5), (5, 8), (8, 10)):
        acc = None
        for pair in range(5):
            lhs = []
            for tap in range(2 * pair, min(2 * pair + 2, 9)):
                dh, dw = tap // 3, tap % 3
                src = xs8 if dh == 1 else xs0
                top = 16 if dh == 2 else 0
                lhs.append(src[lo + dw : hi + dw, top : top + MID_COL].reshape((hi - lo) * MID_COL, C1))
            lhs = jnp.concatenate(lhs, axis=1) if len(lhs) > 1 else lhs[0]
            term = dot(lhs, w1_mat[pair * 256 : pair * 256 + lhs.shape[1], :])
            acc = term if acc is None else acc + term
        act = jnp.maximum(acc + b1_loc[...], 0.0).reshape(hi - lo, MID_COL, C2)
        for half in range(2):
            part = slice(half * 128, half * 128 + 128)
            real = jnp.where(inside[lo:hi] > 0.0, act[:, :, part], 0.0)
            ys0[lo:hi, :, part] = real.astype(jnp.bfloat16)
            ys8[lo:hi, :, part] = real[:, 8:136].astype(jnp.bfloat16)

    for lo in range(0, 8, 2):
        acc = None
        for tap in range(9):
            dh, dw = tap // 3, tap % 3
            src = ys8 if dh == 1 else ys0
            top = 16 if dh == 2 else 0
            term = dot(src[lo + dw : lo + dw + 2, top : top + 128].reshape(256, C2), w2_mat[dh, dw])
            acc = term if acc is None else acc + term
        full = acc + b2_loc[...]
        for w in range(2):
            for half in range(2):
                res[half, (lo + w) * OUT_COL : (lo + w) * OUT_COL + 128] = full[w * 128 : w * 128 + 128, half * 128 : half * 128 + 128]
    for n in range(8):
        for h in range(16):
            for half in range(2):
                out_ref[n, h, :, half * 128 : half * 128 + 128] = res.at[half][pl.ds(h * 8 + n, 8, stride=OUT_COL), :]

    drain(r_w, send_w)
    drain(s_x, send_x)
    swap.wait_send()


def put_out(out_vmem, out_hbm, sem):
    put = pltpu.make_async_copy(out_vmem, out_hbm, sem)
    put.start()
    put.wait()


def solution(mesh):
    def run_local(x_in, w_conv1, b_conv1, w_conv2, b_conv2):
        bf, f32 = jnp.bfloat16, jnp.float32
        vmem = pl.BlockSpec(memory_space=pltpu.VMEM)
        hbm = pl.BlockSpec(memory_space=pltpu.HBM)
        dma = pltpu.SemaphoreType.DMA
        operands = (x_in.reshape(x_in.shape[:3]), w_conv1.reshape(3, 3, C2), b_conv1.reshape(1, C2), w_conv2, b_conv2.reshape(1, C2))
        out = pl.pallas_call(
            kernel,
            name="conv_pair",
            out_shape=jax.ShapeDtypeStruct((8, 16, 8, C2), f32),
            in_specs=[hbm] * 5,
            out_specs=vmem,
            scratch_shapes=[
                pltpu.VMEM((8, 128, 128), bf),
                pltpu.VMEM((3, 3, C2), bf),
                pltpu.VMEM((1, C2), f32),
                pltpu.VMEM((1, C2), f32),
                pltpu.VMEM((3, 3, C2, C2), bf),
                pltpu.VMEM((128, 1024), bf),
                pltpu.VMEM((1024, 2048), bf),
                pltpu.VMEM((256, 1024), bf),
                pltpu.VMEM((256, 256), bf),
                pltpu.VMEM((2, 5, 2, 128), bf),
                pltpu.VMEM((N_DEV, 2, 8, 128), bf),
                pltpu.VMEM((N_DEV, 5, 2, 128), bf),
                pltpu.VMEM((N_DEV, 5, 2, 128), bf),
                pltpu.VMEM((N_DEV, 2, 8, 128), bf),
                pltpu.VMEM((9 * C1, C2), bf),
                pltpu.VMEM((2, N_DEV * 8, 128), f32),
                pltpu.VMEM((3, 128, 128), f32),
                pltpu.VMEM((12, COL, C1), bf),
                pltpu.VMEM((12, MID_COL, C1), bf),
                pltpu.VMEM((10, MID_COL, C2), bf),
                pltpu.VMEM((10, 128, C2), bf),
                pltpu.VMEM((10, MID_COL, 128), f32),
                pltpu.VMEM((2, 8 * OUT_COL, 128), f32),
                dma, dma, pltpu.SemaphoreType.DMA((2,)), dma,
                dma, dma, dma, dma, dma, dma,
            ],
            compiler_params=pltpu.CompilerParams(collective_id=0, has_side_effects=True, vmem_limit_bytes=24 << 20),
        )(*(pltpu.with_memory_space_constraint(a, pltpu.HBM) for a in operands))
        return pl.pallas_call(
            put_out,
            name="put_out",
            out_shape=jax.ShapeDtypeStruct((8, 16, 8, C2), f32),
            in_specs=[vmem],
            out_specs=hbm,
            scratch_shapes=[dma],
            compiler_params=pltpu.CompilerParams(vmem_limit_bytes=24 << 20),
        )(out)

    return jax.shard_map(
        run_local,
        mesh=mesh,
        in_specs=(P("data", None, None, GROUP_AXES), P(None, None, GROUP_AXES, None), P(), P(), P()),
        out_specs=P("data", "model", "cols", None),
        check_vma=False,
    )
```

```python
import collections
import functools

import jax
import jax.numpy as jnp
from jax import lax
from jax.experimental import pallas as pl
from jax.experimental.pallas import tpu as pltpu
from jax.sharding import PartitionSpec as P

MESH = pl.DeviceIdType.MESH
GROUP_AXES = ("model", "cols")

N_DEV = 128
N_COLS = 16
COL = 160
MID_COL = 144
OUT_COL = 40
C1 = 128
C2 = 256
HOPS = (0, 1, 2, 1)


def greet_order():
    shifts = [(dx, dy, dz) for dx in range(4) for dy in range(4) for dz in range(4)][1:]
    return sorted(shifts, key=lambda s: (-HOPS[s[1]] - HOPS[s[2]], -HOPS[s[0]]))


def send_order():
    def key(msg):
        window, dx, dy, z, dk = msg
        return (z // 2, 11 * (z == 1) + 100 * window - 10 * HOPS[dy] + 0.1 * (3, 1, 0, 2)[dx] + 0.01 * dk)

    return sorted(((w, dx, dy, z, dk) for w in range(2) for dx in range(4) for dy in range(4) for z in range(4) for dk in range(2)), key=key)


GREET_ORDER = greet_order()
SEND_ORDER = send_order()
EARLY = ((0,), (2, 3))


def dot(a, b):
    return lax.dot_general(a, b, (((1,), (0,)), ((), ())), preferred_element_type=jnp.float32)


def kernel(x_hbm, w1_hbm, b1_hbm, w2_hbm, b2_hbm, out_ref, ys0, ys8, w2_mat,
           x_loc, w1_loc, b1_loc, b2_loc, turned, pick, sel, place, s_w, s_x, r_w, r_w2, r_x,
           w1_mat, tmp, edge, xs0, xs8, inside, res,
           heard, sem_x, sem_w1, sem_b, sem_w2, send_w, send_x, send_d, recv_w, recv_x, recv_d):
    m = lax.axis_index("model")
    c = lax.axis_index("cols")
    me = m * N_COLS + c
    core = m % 2

    get_x = pltpu.make_async_copy(x_hbm, x_loc, sem_x)
    get_x.start()
    get_w1 = pltpu.make_async_copy(w1_hbm, w1_loc, sem_w1)
    get_w1.start()
    get_b = (pltpu.make_async_copy(b1_hbm, b1_loc, sem_b.at[0]), pltpu.make_async_copy(b2_hbm, b2_loc, sem_b.at[1]))
    for get in get_b:
        get.start()
    get_w2 = pltpu.make_async_copy(w2_hbm, w2_mat, sem_w2)
    get_w2.start()

    cores = (core, 1 - core)
    models = [[((m // 2 + dx) % 4) * 2 + k for k in cores] for dx in range(4)]
    ys = [(c % 4 + dy) % 4 for dy in range(4)]
    my_z = c // 4
    zs = [((my_z + dz) % 4) * 4 for dz in range(4)]

    barrier = pltpu.get_barrier_semaphore()
    part = my_z // 2
    partner = {"model": m + 1 - 2 * core, "cols": c}
    for dx, dy, dz in GREET_ORDER:
        to = {"model": ((m // 2 + dx) % 4) * 2 + part, "cols": zs[dz] + ys[dy]}
        pl.semaphore_signal(barrier, inc=1, device_id=to, device_id_type=MESH)
    pl.semaphore_signal(barrier, inc=1, device_id=partner, device_id_type=MESH)

    def hear(which):
        @pl.when(core == which)
        def _():
            pl.semaphore_wait(barrier, 63 + 2 * ((core + part) % 2))
            pl.semaphore_signal(heard, inc=1, device_id=partner, device_id_type=MESH)

        @pl.when(core != which)
        def _():
            pl.semaphore_wait(heard, 1)

    for blk in range(4):
        lane = blk * 512 + lax.broadcasted_iota(jnp.int32, (1, 512), 1)
        img = lane % 8
        if blk < 2:
            row = (lane // 128) * 16 + (lane // 8) % 16
        else:
            h = (lane // 8) % 4
            row = (lane // 128 - 8) * 16 + h - 2 + jnp.where(h >= 2, 16, 0)
        at = jnp.where((row >= 0) & (row < 128), img * 128 + row, -1)
        for pair in range(4):
            rows = pair * 256 + lax.broadcasted_iota(jnp.int32, (256, 512), 0)
            pick[pair * 256 : pair * 256 + 256, blk * 512 : blk * 512 + 512] = jnp.where(rows == at, 1.0, 0.0).astype(jnp.bfloat16)
    r_id = lax.broadcasted_iota(jnp.int32, (256, 256), 0)
    k_id = lax.broadcasted_iota(jnp.int32, (256, 256), 1)
    first = (r_id // 16) * 8 - 2
    s_id = r_id % 16
    main = (s_id < 12) & (k_id == first + s_id) & (k_id < 128)
    from_col = first + 4 * (s_id - 12)
    border = (s_id >= 12) & (s_id < 15) & (k_id >= 128 + jnp.maximum(from_col, 0)) & (k_id < 132 + from_col)
    place[...] = jnp.where(main | border, 1.0, 0.0).astype(jnp.bfloat16)
    get_w1.wait()
    for k in range(2):
        for j in range(4):
            tap = 4 * k + j
            s_w[k, j] = jnp.concatenate([w1_loc[tap // 3, tap % 3 : tap % 3 + 1, half * 128 : half * 128 + 128] for half in range(2)])
        last = w1_loc[2, 2:3, k * 128 : k * 128 + 128]
        s_w[k, 4] = jnp.concatenate([last, jnp.zeros_like(last)])

    get_x.wait()
    for n in range(8):
        turned[:, n * 128 : n * 128 + 128] = x_loc[n].T
    w_id = lax.broadcasted_iota(jnp.int32, (128, 256), 0)
    l_id = lax.broadcasted_iota(jnp.int32, (128, 256), 1) % 128
    keep = (l_id // 32) == ((w_id + 2) % 4)
    for blk in range(8):
        z = None
        for pair in range(4):
            term = dot(turned[:, pair * 256 : pair * 256 + 256], pick[pair * 256 : pair * 256 + 256, blk * 256 : blk * 256 + 256])
            z = term if z is None else z + term
        if blk >= 4:
            z = jnp.where(keep, z, 0.0)
        top = 0 if blk < 4 else 128
        sel[top : top + 128, (blk % 4) * 256 : (blk % 4) * 256 + 256] = z.astype(jnp.bfloat16)
    for blk in range(4):
        t = dot(place[...], sel[:, blk * 256 : blk * 256 + 256])
        for r in range(2):
            tiles = t[:, r * 128 : r * 128 + 128].reshape(16, 2, 8, 128).astype(jnp.bfloat16)
            s_x[(blk * 2 + r) * 16 : (blk * 2 + r) * 16 + 16] = tiles


    def send(src, dst, send_sem, recv_sem, pm, pc):
        pltpu.make_async_remote_copy(src_ref=src, dst_ref=dst, send_sem=send_sem, recv_sem=recv_sem,
                                     device_id={"model": pm, "cols": pc}, device_id_type=MESH).start()

    for step, (window, dx, dy, z, dk) in enumerate(SEND_ORDER):
        if step % N_DEV == 0:
            hear(step // N_DEV)
        if window and SEND_ORDER[step - 1][0] == 0:
            for first_z in EARLY[step // N_DEV]:
                for k in (1, 0):
                    def send_early(pm=k, pc=first_z * 4):
                        send(s_x.at[pm * N_COLS + pc], r_x.at[me], send_x, recv_x, pm, pc)
                    pl.when(me != k * N_COLS + first_z * 4)(send_early)
        pm, pc = models[dx][dk], z * 4 + ys[dy]

        def send_one(window=window, pm=pm, pc=pc, pk=cores[dk]):
            if window:
                send(s_x.at[pm * N_COLS + pc], r_x.at[me], send_x, recv_x, pm, pc)
            else:
                send(s_w.at[pk], r_w.at[me], send_w, recv_w, pm, pc)

        if window and z in EARLY[z // 2]:
            sent = models[dx][0] // 2 + ys[dy] == 0
            skip = sent | (my_z == z) if dx == dy == dk == 0 else sent
            pl.when(jnp.logical_not(skip))(send_one)
        elif dx == dy == dk == 0:
            pl.when(my_z != z)(send_one)
        else:
            send_one()
    r_w[pl.ds(me, 1)] = s_w[pl.ds(core, 1)]
    r_x[pl.ds(me, 1)] = s_x[pl.ds(me, 1)]

    at_row = m * 16 - 1 + lax.broadcasted_iota(jnp.int32, (10, MID_COL, 128), 1) // 8
    at_col = c * 8 - 1 + lax.broadcasted_iota(jnp.int32, (10, MID_COL, 128), 0)
    inside[...] = jnp.where((at_row >= 0) & (at_row < 128) & (at_col >= 0) & (at_col < 128), 1.0, 0.0)

    def drain(ref, sem):
        part = ref.at[pl.ds(0, N_DEV - 1)]
        pltpu.make_async_copy(part, part, sem).wait()

    def unpack_w(ref, k):
        for j in range(5):
            tmp[0, 0 : 2 * N_DEV] = ref[:, j].astype(jnp.float32).reshape(N_DEV * 2, 128)
            for half in range(2 if j < 4 else 1):
                rows = tmp.at[0][pl.ds(half, N_DEV, stride=2), :].astype(jnp.bfloat16)
                if j < 4:
                    at = pl.multiple_of((4 * k + j) * C1, C1)
                    w1_mat[pl.ds(at, C1), half * 128 : half * 128 + 128] = rows
                else:
                    w1_mat[8 * C1 : 9 * C1, pl.ds(pl.multiple_of(k * 128, 128), 128)] = rows

    drain(r_w, recv_w)
    swap = pltpu.make_async_remote_copy(src_ref=r_w, dst_ref=r_w2, send_sem=send_d, recv_sem=recv_d,
                                        device_id=partner, device_id_type=MESH)
    swap.start()
    unpack_w(r_w, core)
    swap.wait_recv()
    unpack_w(r_w2, 1 - core)
    for get in get_b:
        get.wait()
    get_w2.wait()

    drain(r_x, recv_x)
    for half in range(2):
        tmp[half] = r_x[:, half].astype(jnp.float32).reshape(N_DEV * 8, 128)

    def pixels(s):
        return tmp.at[s // 8][pl.ds(s % 8, N_DEV, stride=8), :].T

    for s in range(12, 15):
        edge[s - 12] = pixels(s)
    for w in range(12):
        top = (w % 4) * 32
        col = jnp.concatenate([edge[w // 4, top : top + 16], pixels(w), edge[w // 4, top + 16 : top + 32]])
        xs0[w] = col.astype(jnp.bfloat16)
        xs8[w] = col[8 : 8 + MID_COL].astype(jnp.bfloat16)

    before = None
    for top, rows in ((0, 48), (48, 32), (80, 32), (112, 32)):
        acc = None
        for pair in range(5):
            lhs = []
            for tap in range(2 * pair, min(2 * pair + 2, 9)):
                dh, dw = tap // 3, tap % 3
                src = xs8 if dh == 1 else xs0
                at = top + (16 if dh == 2 else 0)
                lhs.append(src[dw : dw + 10, at : at + rows].reshape(10 * rows, C1))
            lhs = jnp.concatenate(lhs, axis=1) if len(lhs) > 1 else lhs[0]
            term = dot(lhs, w1_mat[pair * 256 : pair * 256 + lhs.shape[1], :])
            acc = term if acc is None else acc + term
        act = jnp.maximum(acc + b1_loc[...], 0.0).reshape(10, rows, C2)
        ok = inside[:, top : top + rows] > 0.0
        real = [jnp.where(ok, act[:, :, half * 128 : half * 128 + 128], 0.0) for half in range(2)]
        for half in range(2):
            part = slice(half * 128, half * 128 + 128)
            ys0[:, top : top + rows, part] = real[half].astype(jnp.bfloat16)
            if before is None:
                ys8[:, 0 : rows - 16, part] = real[half][:, 8 : rows - 8].astype(jnp.bfloat16)
            else:
                shifted = jnp.concatenate([before[half], real[half][:, 0 : rows - 8]], axis=1)
                ys8[:, top - 16 : top + rows - 16, part] = shifted.astype(jnp.bfloat16)
        before = [r[:, rows - 8 :] for r in real]

    for blk in range(3):
        conv_two(blk, ys0, ys8, w2_mat, b2_loc, res.at[blk], out_ref)

    drain(r_w, send_w)
    drain(s_x, send_x)
    swap.wait_send()


def conv_two(blk, ys0, ys8, w2_mat, b2_ref, res, out_ref):
    acc = None
    for tap in range(9):
        dh, dw = tap // 3, tap % 3
        src = ys8 if dh == 1 else ys0
        at = blk * 32 + (16 if dh == 2 else 0)
        term = dot(src[dw : dw + 8, at : at + 32].reshape(256, C2), w2_mat[dh, dw])
        acc = term if acc is None else acc + term
    full = acc + b2_ref[...]
    for w in range(8):
        for half in range(2):
            res[half, w * OUT_COL : w * OUT_COL + 32] = full[w * 32 : w * 32 + 32, half * 128 : half * 128 + 128]
    for h in range(4):
        for n in range(8):
            for half in range(2):
                rows = res.at[half][pl.ds(h * 8 + n, 8, stride=OUT_COL), :]
                out_ref[n, (blk * 4) % out_ref.shape[1] + h, :, half * 128 : half * 128 + 128] = rows


def kernel_two(out_a, ys0, ys8, w2_mat, b2_ref, out_hbm, out_b, res, sem):
    put_a = pltpu.make_async_copy(out_a, out_hbm.at[:, 0:12], sem.at[0])
    put_a.start()
    conv_two(3, ys0, ys8, w2_mat, b2_ref, res, out_b)
    put_b = pltpu.make_async_copy(out_b, out_hbm.at[:, 12:16], sem.at[1])
    put_b.start()
    put_a.wait()
    put_b.wait()


def solution(mesh):
    def run_local(x_in, w_conv1, b_conv1, w_conv2, b_conv2):
        bf, f32 = jnp.bfloat16, jnp.float32
        vmem = pl.BlockSpec(memory_space=pltpu.VMEM)
        hbm = pl.BlockSpec(memory_space=pltpu.HBM)
        dma = pltpu.SemaphoreType.DMA
        operands = (x_in.reshape(x_in.shape[:3]), w_conv1.reshape(3, 3, C2), b_conv1.reshape(1, C2), w_conv2, b_conv2.reshape(1, C2))
        out_a, ys0, ys8, w2 = pl.pallas_call(
            kernel,
            name="conv_pair",
            out_shape=[
                jax.ShapeDtypeStruct((8, 12, 8, C2), f32),
                jax.ShapeDtypeStruct((10, MID_COL, C2), bf),
                jax.ShapeDtypeStruct((10, 128, C2), bf),
                jax.ShapeDtypeStruct((3, 3, C2, C2), bf),
            ],
            in_specs=[hbm] * 5,
            out_specs=[vmem] * 4,
            scratch_shapes=[
                pltpu.VMEM((8, 128, 128), bf),
                pltpu.VMEM((3, 3, C2), bf),
                pltpu.VMEM((1, C2), f32),
                pltpu.VMEM((1, C2), f32),
                pltpu.VMEM((128, 1024), bf),
                pltpu.VMEM((1024, 2048), bf),
                pltpu.VMEM((256, 1024), bf),
                pltpu.VMEM((256, 256), bf),
                pltpu.VMEM((2, 5, 2, 128), bf),
                pltpu.VMEM((N_DEV, 2, 8, 128), bf),
                pltpu.VMEM((N_DEV, 5, 2, 128), bf),
                pltpu.VMEM((N_DEV, 5, 2, 128), bf),
                pltpu.VMEM((N_DEV, 2, 8, 128), bf),
                pltpu.VMEM((9 * C1, C2), bf),
                pltpu.VMEM((2, N_DEV * 8, 128), f32),
                pltpu.VMEM((3, 128, 128), f32),
                pltpu.VMEM((12, COL, C1), bf),
                pltpu.VMEM((12, MID_COL, C1), bf),
                pltpu.VMEM((10, MID_COL, 128), f32),
                pltpu.VMEM((3, 2, 8 * OUT_COL, 128), f32),
                pltpu.SemaphoreType.REGULAR, dma, dma, pltpu.SemaphoreType.DMA((2,)), dma,
                dma, dma, dma, dma, dma, dma,
            ],
            compiler_params=pltpu.CompilerParams(collective_id=0, has_side_effects=True, vmem_limit_bytes=24 << 20),
        )(*(pltpu.with_memory_space_constraint(a, pltpu.HBM) for a in operands))
        return pl.pallas_call(
            kernel_two,
            name="conv_last",
            out_shape=jax.ShapeDtypeStruct((8, 16, 8, C2), f32),
            in_specs=[vmem] * 5,
            out_specs=hbm,
            scratch_shapes=[pltpu.VMEM((8, 4, 8, C2), f32), pltpu.VMEM((2, 8 * OUT_COL, 128), f32), pltpu.SemaphoreType.DMA((2,))],
            compiler_params=pltpu.CompilerParams(vmem_limit_bytes=24 << 20),
        )(out_a, ys0, ys8, w2, operands[-1])

    return jax.shard_map(
        run_local,
        mesh=mesh,
        in_specs=(P("data", None, None, GROUP_AXES), P(None, None, GROUP_AXES, None), P(), P(), P()),
        out_specs=P("data", "model", "cols", None),
        check_vma=False,
    )
```

```python
import collections
import functools

import jax
import jax.numpy as jnp
from jax import lax
from jax.experimental import pallas as pl
from jax.experimental.pallas import tpu as pltpu
from jax.sharding import PartitionSpec as P

MESH = pl.DeviceIdType.MESH
GROUP_AXES = ("model", "cols")

N_DEV = 128
N_COLS = 16
COL = 160
MID_COL = 144
OUT_COL = 40
C1 = 128
C2 = 256
HOPS = (0, 1, 2, 1)


def greet_order():
    shifts = [(dx, dy, dz) for dx in range(4) for dy in range(4) for dz in range(4)][1:]
    return sorted(shifts, key=lambda s: (-HOPS[s[1]] - HOPS[s[2]], -HOPS[s[0]]))


def send_order():
    def key(msg):
        window, dx, dy, z, dk = msg
        return (z > 0, 11 * (z > 1) + 100 * window - 10 * HOPS[dy] + 0.1 * (3, 1, 0, 2)[dx] + 0.01 * dk)

    return sorted(((w, dx, dy, z, dk) for w in range(2) for dx in range(4) for dy in range(4) for z in range(4) for dk in range(2)), key=key)


GREET_ORDER = greet_order()
SEND_ORDER = send_order()
SPLIT = 1
EARLY = {32: 0, 160: 1}


def dot(a, b):
    return lax.dot_general(a, b, (((1,), (0,)), ((), ())), preferred_element_type=jnp.float32)


def kernel(x_hbm, w1_hbm, b1_hbm, w2_hbm, b2_hbm, out_ref, ys0, ys8, w2_mat,
           x_loc, w1_loc, b1_loc, b2_loc, turned, pick, sel, place, s_w, s_x, r_w, r_w2, r_x,
           w1_mat, tmp, edge, xs0, xs8, inside, res,
           heard, sem_x, sem_w1, sem_b, sem_w2, send_w, send_x, send_d, recv_w, recv_x, recv_d):
    m = lax.axis_index("model")
    c = lax.axis_index("cols")
    me = m * N_COLS + c
    core = m % 2

    get_x = pltpu.make_async_copy(x_hbm, x_loc, sem_x)
    get_x.start()
    get_w1 = pltpu.make_async_copy(w1_hbm, w1_loc, sem_w1)
    get_w1.start()
    get_b = (pltpu.make_async_copy(b1_hbm, b1_loc, sem_b.at[0]), pltpu.make_async_copy(b2_hbm, b2_loc, sem_b.at[1]))
    for get in get_b:
        get.start()
    get_w2 = pltpu.make_async_copy(w2_hbm, w2_mat, sem_w2)
    get_w2.start()

    cores = (core, 1 - core)
    models = [[((m // 2 + dx) % 4) * 2 + k for k in cores] for dx in range(4)]
    ys = [(c % 4 + dy) % 4 for dy in range(4)]
    my_z = c // 4
    zs = [((my_z + dz) % 4) * 4 for dz in range(4)]

    barrier = pltpu.get_barrier_semaphore()
    part = (my_z + 4 - SPLIT) // 4
    partner = {"model": m + 1 - 2 * core, "cols": c}
    for dx, dy, dz in GREET_ORDER:
        to = {"model": ((m // 2 + dx) % 4) * 2 + part, "cols": zs[dz] + ys[dy]}
        pl.semaphore_signal(barrier, inc=1, device_id=to, device_id_type=MESH)
    pl.semaphore_signal(barrier, inc=1, device_id=partner, device_id_type=MESH)

    def hear(which):
        @pl.when(core == which)
        def _():
            pl.semaphore_wait(barrier, (SPLIT * 32, 128 - SPLIT * 32)[which] - 1 + 2 * ((core + part) % 2))
            pl.semaphore_signal(heard, inc=1, device_id=partner, device_id_type=MESH)

        @pl.when(core != which)
        def _():
            pl.semaphore_wait(heard, 1)

    for blk in range(4):
        lane = blk * 512 + lax.broadcasted_iota(jnp.int32, (1, 512), 1)
        img = lane % 8
        if blk < 2:
            row = (lane // 128) * 16 + (lane // 8) % 16
        else:
            h = (lane // 8) % 4
            row = (lane // 128 - 8) * 16 + h - 2 + jnp.where(h >= 2, 16, 0)
        at = jnp.where((row >= 0) & (row < 128), img * 128 + row, -1)
        for pair in range(4):
            rows = pair * 256 + lax.broadcasted_iota(jnp.int32, (256, 512), 0)
            pick[pair * 256 : pair * 256 + 256, blk * 512 : blk * 512 + 512] = jnp.where(rows == at, 1.0, 0.0).astype(jnp.bfloat16)
    r_id = lax.broadcasted_iota(jnp.int32, (256, 256), 0)
    k_id = lax.broadcasted_iota(jnp.int32, (256, 256), 1)
    first = (r_id // 16) * 8 - 2
    s_id = r_id % 16
    main = (s_id < 12) & (k_id == first + s_id) & (k_id < 128)
    from_col = first + 4 * (s_id - 12)
    border = (s_id >= 12) & (s_id < 15) & (k_id >= 128 + jnp.maximum(from_col, 0)) & (k_id < 132 + from_col)
    place[...] = jnp.where(main | border, 1.0, 0.0).astype(jnp.bfloat16)
    get_w1.wait()
    for k in range(2):
        for j in range(4):
            tap = 4 * k + j
            s_w[k, j] = jnp.concatenate([w1_loc[tap // 3, tap % 3 : tap % 3 + 1, half * 128 : half * 128 + 128] for half in range(2)])
        last = w1_loc[2, 2:3, k * 128 : k * 128 + 128]
        s_w[k, 4] = jnp.concatenate([last, jnp.zeros_like(last)])

    get_x.wait()
    for n in range(8):
        turned[:, n * 128 : n * 128 + 128] = x_loc[n].T
    w_id = lax.broadcasted_iota(jnp.int32, (128, 256), 0)
    l_id = lax.broadcasted_iota(jnp.int32, (128, 256), 1) % 128
    keep = (l_id // 32) == ((w_id + 2) % 4)
    for blk in range(8):
        z = None
        for pair in range(4):
            term = dot(turned[:, pair * 256 : pair * 256 + 256], pick[pair * 256 : pair * 256 + 256, blk * 256 : blk * 256 + 256])
            z = term if z is None else z + term
        if blk >= 4:
            z = jnp.where(keep, z, 0.0)
        top = 0 if blk < 4 else 128
        sel[top : top + 128, (blk % 4) * 256 : (blk % 4) * 256 + 256] = z.astype(jnp.bfloat16)
    for blk in range(4):
        t = dot(place[...], sel[:, blk * 256 : blk * 256 + 256])
        for r in range(2):
            tiles = t[:, r * 128 : r * 128 + 128].reshape(16, 2, 8, 128).astype(jnp.bfloat16)
            s_x[(blk * 2 + r) * 16 : (blk * 2 + r) * 16 + 16] = tiles


    def send(src, dst, send_sem, recv_sem, pm, pc):
        pltpu.make_async_remote_copy(src_ref=src, dst_ref=dst, send_sem=send_sem, recv_sem=recv_sem,
                                     device_id={"model": pm, "cols": pc}, device_id_type=MESH).start()

    for step, (window, dx, dy, z, dk) in enumerate(SEND_ORDER):
        if step in (0, SPLIT * 64):
            hear(min(step, 1))
        if step in EARLY:
            for k in (1, 0):
                def send_early(pm=k, pc=EARLY[step] * 4):
                    send(s_x.at[pm * N_COLS + pc], r_x.at[me], send_x, recv_x, pm, pc)
                pl.when(me != k * N_COLS + EARLY[step] * 4)(send_early)
        pm, pc = models[dx][dk], z * 4 + ys[dy]

        def send_one(window=window, pm=pm, pc=pc, pk=cores[dk]):
            if window:
                send(s_x.at[pm * N_COLS + pc], r_x.at[me], send_x, recv_x, pm, pc)
            else:
                send(s_w.at[pk], r_w.at[me], send_w, recv_w, pm, pc)

        if window and z in EARLY.values():
            sent = models[dx][0] // 2 + ys[dy] == 0
            skip = sent | (my_z == z) if dx == dy == dk == 0 else sent
            pl.when(jnp.logical_not(skip))(send_one)
        elif dx == dy == dk == 0:
            pl.when(my_z != z)(send_one)
        else:
            send_one()
    r_w[pl.ds(me, 1)] = s_w[pl.ds(core, 1)]
    r_x[pl.ds(me, 1)] = s_x[pl.ds(me, 1)]

    at_row = m * 16 - 1 + lax.broadcasted_iota(jnp.int32, (10, MID_COL, 128), 1) // 8
    at_col = c * 8 - 1 + lax.broadcasted_iota(jnp.int32, (10, MID_COL, 128), 0)
    inside[...] = jnp.where((at_row >= 0) & (at_row < 128) & (at_col >= 0) & (at_col < 128), 1.0, 0.0)

    def drain(ref, sem):
        part = ref.at[pl.ds(0, N_DEV - 1)]
        pltpu.make_async_copy(part, part, sem).wait()

    def unpack_w(ref, k):
        for j in range(5):
            tmp[0, 0 : 2 * N_DEV] = ref[:, j].astype(jnp.float32).reshape(N_DEV * 2, 128)
            for half in range(2 if j < 4 else 1):
                rows = tmp.at[0][pl.ds(half, N_DEV, stride=2), :].astype(jnp.bfloat16)
                if j < 4:
                    at = pl.multiple_of((4 * k + j) * C1, C1)
                    w1_mat[pl.ds(at, C1), half * 128 : half * 128 + 128] = rows
                else:
                    w1_mat[8 * C1 : 9 * C1, pl.ds(pl.multiple_of(k * 128, 128), 128)] = rows

    drain(r_w, recv_w)
    swap = pltpu.make_async_remote_copy(src_ref=r_w, dst_ref=r_w2, send_sem=send_d, recv_sem=recv_d,
                                        device_id=partner, device_id_type=MESH)
    swap.start()
    unpack_w(r_w, core)
    swap.wait_recv()
    unpack_w(r_w2, 1 - core)
    for get in get_b:
        get.wait()
    get_w2.wait()

    drain(r_x, recv_x)
    for half in range(2):
        tmp[half] = r_x[:, half].astype(jnp.float32).reshape(N_DEV * 8, 128)

    def pixels(s):
        return tmp.at[s // 8][pl.ds(s % 8, N_DEV, stride=8), :].T

    for s in range(12, 15):
        edge[s - 12] = pixels(s)
    for w in range(12):
        top = (w % 4) * 32
        col = jnp.concatenate([edge[w // 4, top : top + 16], pixels(w), edge[w // 4, top + 16 : top + 32]])
        xs0[w] = col.astype(jnp.bfloat16)
        xs8[w] = col[8 : 8 + MID_COL].astype(jnp.bfloat16)

    before = None
    for top, rows in ((0, 48), (48, 32), (80, 32), (112, 32)):
        acc = None
        for pair in range(5):
            lhs = []
            for tap in range(2 * pair, min(2 * pair + 2, 9)):
                dh, dw = tap // 3, tap % 3
                src = xs8 if dh == 1 else xs0
                at = top + (16 if dh == 2 else 0)
                lhs.append(src[dw : dw + 10, at : at + rows].reshape(10 * rows, C1))
            lhs = jnp.concatenate(lhs, axis=1) if len(lhs) > 1 else lhs[0]
            term = dot(lhs, w1_mat[pair * 256 : pair * 256 + lhs.shape[1], :])
            acc = term if acc is None else acc + term
        act = jnp.maximum(acc + b1_loc[...], 0.0).reshape(10, rows, C2)
        ok = inside[:, top : top + rows] > 0.0
        real = [jnp.where(ok, act[:, :, half * 128 : half * 128 + 128], 0.0) for half in range(2)]
        for half in range(2):
            part = slice(half * 128, half * 128 + 128)
            ys0[:, top : top + rows, part] = real[half].astype(jnp.bfloat16)
            if before is None:
                ys8[:, 0 : rows - 16, part] = real[half][:, 8 : rows - 8].astype(jnp.bfloat16)
            else:
                shifted = jnp.concatenate([before[half], real[half][:, 0 : rows - 8]], axis=1)
                ys8[:, top - 16 : top + rows - 16, part] = shifted.astype(jnp.bfloat16)
        before = [r[:, rows - 8 :] for r in real]

    for blk in range(3):
        conv_two(blk, ys0, ys8, w2_mat, b2_loc, res.at[blk], out_ref)

    drain(r_w, send_w)
    drain(s_x, send_x)
    swap.wait_send()


def conv_two(blk, ys0, ys8, w2_mat, b2_ref, res, out_ref):
    acc = None
    for tap in range(9):
        dh, dw = tap // 3, tap % 3
        src = ys8 if dh == 1 else ys0
        at = blk * 32 + (16 if dh == 2 else 0)
        term = dot(src[dw : dw + 8, at : at + 32].reshape(256, C2), w2_mat[dh, dw])
        acc = term if acc is None else acc + term
    full = acc + b2_ref[...]
    for w in range(8):
        for half in range(2):
            res[half, w * OUT_COL : w * OUT_COL + 32] = full[w * 32 : w * 32 + 32, half * 128 : half * 128 + 128]
    for h in range(4):
        for n in range(8):
            for half in range(2):
                rows = res.at[half][pl.ds(h * 8 + n, 8, stride=OUT_COL), :]
                out_ref[n, (blk * 4) % out_ref.shape[1] + h, :, half * 128 : half * 128 + 128] = rows


def kernel_two(out_a, ys0, ys8, w2_mat, b2_ref, out_hbm, out_b, res, sem):
    put_a = pltpu.make_async_copy(out_a, out_hbm.at[:, 0:12], sem.at[0])
    put_a.start()
    conv_two(3, ys0, ys8, w2_mat, b2_ref, res, out_b)
    put_b = pltpu.make_async_copy(out_b, out_hbm.at[:, 12:16], sem.at[1])
    put_b.start()
    put_a.wait()
    put_b.wait()


def solution(mesh):
    def run_local(x_in, w_conv1, b_conv1, w_conv2, b_conv2):
        bf, f32 = jnp.bfloat16, jnp.float32
        vmem = pl.BlockSpec(memory_space=pltpu.VMEM)
        hbm = pl.BlockSpec(memory_space=pltpu.HBM)
        dma = pltpu.SemaphoreType.DMA
        operands = (x_in.reshape(x_in.shape[:3]), w_conv1.reshape(3, 3, C2), b_conv1.reshape(1, C2), w_conv2, b_conv2.reshape(1, C2))
        out_a, ys0, ys8, w2 = pl.pallas_call(
            kernel,
            name="conv_pair",
            out_shape=[
                jax.ShapeDtypeStruct((8, 12, 8, C2), f32),
                jax.ShapeDtypeStruct((10, MID_COL, C2), bf),
                jax.ShapeDtypeStruct((10, 128, C2), bf),
                jax.ShapeDtypeStruct((3, 3, C2, C2), bf),
            ],
            in_specs=[hbm] * 5,
            out_specs=[vmem] * 4,
            scratch_shapes=[
                pltpu.VMEM((8, 128, 128), bf),
                pltpu.VMEM((3, 3, C2), bf),
                pltpu.VMEM((1, C2), f32),
                pltpu.VMEM((1, C2), f32),
                pltpu.VMEM((128, 1024), bf),
                pltpu.VMEM((1024, 2048), bf),
                pltpu.VMEM((256, 1024), bf),
                pltpu.VMEM((256, 256), bf),
                pltpu.VMEM((2, 5, 2, 128), bf),
                pltpu.VMEM((N_DEV, 2, 8, 128), bf),
                pltpu.VMEM((N_DEV, 5, 2, 128), bf),
                pltpu.VMEM((N_DEV, 5, 2, 128), bf),
                pltpu.VMEM((N_DEV, 2, 8, 128), bf),
                pltpu.VMEM((9 * C1, C2), bf),
                pltpu.VMEM((2, N_DEV * 8, 128), f32),
                pltpu.VMEM((3, 128, 128), f32),
                pltpu.VMEM((12, COL, C1), bf),
                pltpu.VMEM((12, MID_COL, C1), bf),
                pltpu.VMEM((10, MID_COL, 128), f32),
                pltpu.VMEM((3, 2, 8 * OUT_COL, 128), f32),
                pltpu.SemaphoreType.REGULAR, dma, dma, pltpu.SemaphoreType.DMA((2,)), dma,
                dma, dma, dma, dma, dma, dma,
            ],
            compiler_params=pltpu.CompilerParams(collective_id=0, has_side_effects=True, vmem_limit_bytes=24 << 20),
        )(*(pltpu.with_memory_space_constraint(a, pltpu.HBM) for a in operands))
        return pl.pallas_call(
            kernel_two,
            name="conv_last",
            out_shape=jax.ShapeDtypeStruct((8, 16, 8, C2), f32),
            in_specs=[vmem] * 5,
            out_specs=hbm,
            scratch_shapes=[pltpu.VMEM((8, 4, 8, C2), f32), pltpu.VMEM((2, 8 * OUT_COL, 128), f32), pltpu.SemaphoreType.DMA((2,))],
            compiler_params=pltpu.CompilerParams(vmem_limit_bytes=24 << 20),
        )(out_a, ys0, ys8, w2, operands[-1])

    return jax.shard_map(
        run_local,
        mesh=mesh,
        in_specs=(P("data", None, None, GROUP_AXES), P(None, None, GROUP_AXES, None), P(), P(), P()),
        out_specs=P("data", "model", "cols", None),
        check_vma=False,
    )
```

```python
import collections
import functools

import jax
import jax.numpy as jnp
from jax import lax
from jax.experimental import pallas as pl
from jax.experimental.pallas import tpu as pltpu
from jax.sharding import PartitionSpec as P

MESH = pl.DeviceIdType.MESH
GROUP_AXES = ("model", "cols")

N_DEV = 128
N_COLS = 16
COL = 160
MID_COL = 144
OUT_COL = 40
BLOCKS = ((0, 4), (4, 4), (8, 4), (12, 2))
LAST = 14
C1 = 128
C2 = 256
HOPS = (0, 1, 2, 1)


def greet_order():
    shifts = [(dx, dy, dz) for dx in range(4) for dy in range(4) for dz in range(4)][1:]
    return sorted(shifts, key=lambda s: (-HOPS[s[1]] - HOPS[s[2]], -HOPS[s[0]]))


GREET_ORDER = greet_order()
SEND_ORDER = ((
    16, 112, 80, 48, 8, 104, 24, 72, 120, 40, 88, 56, 0, 96, 64, 32, 145, 144, 241, 240, 209, 208, 177, 176,
    137, 136, 233, 232, 153, 152, 201, 249, 200, 248, 169, 168, 217, 216, 185, 184, 129, 128, 225, 224, 193, 192, 161, 160,
), (
    18, 114, 82, 50, 10, 106, 26, 20, 22, 74, 122, 42, 116, 118, 90, 58, 84, 86, 52, 54, 12, 14, 2, 108,
    110, 28, 30, 98, 76, 78, 124, 126, 44, 46, 66, 34, 92, 94, 60, 62, 4, 6, 100, 102, 68, 70, 36, 38,
    147, 146, 243, 242, 211, 210, 179, 178, 139, 138, 235, 234, 155, 154, 149, 151, 203, 251, 148, 150, 202, 250, 171, 170,
    245, 247, 244, 246, 219, 218, 187, 186, 213, 215, 212, 214, 181, 183, 180, 182, 141, 143, 140, 142, 131, 237, 239, 130,
    236, 238, 157, 159, 227, 156, 158, 226, 205, 207, 253, 255, 204, 206, 252, 254, 173, 175, 172, 174, 195, 194, 163, 162,
    221, 223, 220, 222, 189, 191, 188, 190, 133, 135, 132, 134, 229, 231, 228, 230, 197, 199, 196, 198, 165, 167, 164, 166,
))
EARLY = ({}, {})


def dot(a, b):
    return lax.dot_general(a, b, (((1,), (0,)), ((), ())), preferred_element_type=jnp.float32)


def kernel(x_hbm, w1_hbm, b1_hbm, w2_hbm, b2_hbm, out_ref, ys0, ys8, w2_mat,
           x_loc, w1_loc, b1_loc, b2_loc, turned, pick, sel, place, s_w, s_x, r_w, r_w2, r_x,
           w1_mat, tmp, edge, xs0, xs8, inside, res,
           heard, sem_x, sem_w1, sem_b, sem_w2, send_w, send_x, send_d, recv_w, recv_x, recv_d):
    m = lax.axis_index("model")
    c = lax.axis_index("cols")
    core = m % 2
    chip = m // 2 * N_COLS + c
    me = core * 64 + chip

    get_x = pltpu.make_async_copy(x_hbm, x_loc, sem_x)
    get_x.start()
    get_w1 = pltpu.make_async_copy(w1_hbm, w1_loc, sem_w1)
    get_w1.start()
    get_b = (pltpu.make_async_copy(b1_hbm, b1_loc, sem_b.at[0]), pltpu.make_async_copy(b2_hbm, b2_loc, sem_b.at[1]))
    for get in get_b:
        get.start()
    get_w2 = pltpu.make_async_copy(w2_hbm, w2_mat, sem_w2)
    get_w2.start()

    cores = (core, 1 - core)
    models = [[((m // 2 + dx) % 4) * 2 + k for k in cores] for dx in range(4)]
    ys = [(c % 4 + dy) % 4 for dy in range(4)]
    my_z = c // 4
    zs = [((my_z + dz) % 4) * 4 for dz in range(4)]

    barrier = pltpu.get_barrier_semaphore()
    part = (my_z + 3) // 4
    partner = {"model": m + 1 - 2 * core, "cols": c}
    for dx, dy, dz in GREET_ORDER:
        to = {"model": ((m // 2 + dx) % 4) * 2 + part, "cols": zs[dz] + ys[dy]}
        pl.semaphore_signal(barrier, inc=1, device_id=to, device_id_type=MESH)
    pl.semaphore_signal(barrier, inc=1, device_id=partner, device_id_type=MESH)

    def hear(which):
        @pl.when(core == which)
        def _():
            pl.semaphore_wait(barrier, (32, 96)[which] - 1 + 2 * ((core + part) % 2))
            pl.semaphore_signal(heard, inc=1, device_id=partner, device_id_type=MESH)

        @pl.when(core != which)
        def _():
            pl.semaphore_wait(heard, 1)

    for blk in range(4):
        lane = blk * 512 + lax.broadcasted_iota(jnp.int32, (1, 512), 1)
        img = lane % 8
        if blk < 2:
            row = (lane // 128) * 16 + (lane // 8) % 16
        else:
            h = (lane // 8) % 4
            row = (lane // 128 - 8) * 16 + h - 2 + jnp.where(h >= 2, 16, 0)
        at = jnp.where((row >= 0) & (row < 128), img * 128 + row, -1)
        for pair in range(4):
            rows = pair * 256 + lax.broadcasted_iota(jnp.int32, (256, 512), 0)
            pick[pair * 256 : pair * 256 + 256, blk * 512 : blk * 512 + 512] = jnp.where(rows == at, 1.0, 0.0).astype(jnp.bfloat16)
    r_id = lax.broadcasted_iota(jnp.int32, (256, 256), 0)
    k_id = lax.broadcasted_iota(jnp.int32, (256, 256), 1)
    first = (r_id // 16) * 8 - 2
    s_id = r_id % 16
    main = (s_id < 12) & (k_id == first + s_id) & (k_id < 128)
    from_col = first + 4 * (s_id - 12)
    border = (s_id >= 12) & (s_id < 15) & (k_id >= 128 + jnp.maximum(from_col, 0)) & (k_id < 132 + from_col)
    place[...] = jnp.where(main | border, 1.0, 0.0).astype(jnp.bfloat16)
    get_w1.wait()
    for tap in range(9):
        s_w[tap] = jnp.concatenate([w1_loc[tap // 3, tap % 3 : tap % 3 + 1, half * 128 : half * 128 + 128] for half in range(2)])

    get_x.wait()
    for n in range(8):
        turned[:, n * 128 : n * 128 + 128] = x_loc[n].T
    w_id = lax.broadcasted_iota(jnp.int32, (128, 256), 0)
    l_id = lax.broadcasted_iota(jnp.int32, (128, 256), 1) % 128
    keep = (l_id // 32) == ((w_id + 2) % 4)
    for blk in range(8):
        z = None
        for pair in range(4):
            term = dot(turned[:, pair * 256 : pair * 256 + 256], pick[pair * 256 : pair * 256 + 256, blk * 256 : blk * 256 + 256])
            z = term if z is None else z + term
        if blk >= 4:
            z = jnp.where(keep, z, 0.0)
        top = 0 if blk < 4 else 128
        sel[top : top + 128, (blk % 4) * 256 : (blk % 4) * 256 + 256] = z.astype(jnp.bfloat16)
    for blk in range(4):
        t = dot(place[...], sel[:, blk * 256 : blk * 256 + 256])
        for r in range(2):
            tiles = t[:, r * 128 : r * 128 + 128].reshape(16, 2, 8, 128).astype(jnp.bfloat16)
            s_x[(blk * 2 + r) * 16 : (blk * 2 + r) * 16 + 16] = tiles


    def send(src, dst, send_sem, recv_sem, pm, pc):
        pltpu.make_async_remote_copy(src_ref=src, dst_ref=dst, send_sem=send_sem, recv_sem=recv_sem,
                                     device_id={"model": pm, "cols": pc}, device_id_type=MESH).start()

    early_zs = {z for early in EARLY for layers in early.values() for z in layers}
    for which, order in enumerate(SEND_ORDER):
        hear(which)
        for pos, msg in enumerate(order):
            window, dx, dy, z, dk = msg // 128, msg // 32 % 4, msg // 8 % 4, msg // 2 % 4, msg % 2
            for ez in EARLY[which].get(pos, ()):
                for k in (1, 0):
                    def send_early(pm=k, pc=ez * 4):
                        send(s_x.at[pm * N_COLS + pc], r_x.at[me], send_x, recv_x, pm, pc)
                    pl.when((m != k) | (c != ez * 4))(send_early)
            pm, pc = models[dx][dk], z * 4 + ys[dy]

            def send_one(window=window, pm=pm, pc=pc):
                if window:
                    send(s_x.at[pm * N_COLS + pc], r_x.at[me], send_x, recv_x, pm, pc)
                else:
                    send(s_w, r_w.at[chip], send_w, recv_w, pm, pc)

            conds = []
            if dx == dy == dk == 0:
                conds.append(my_z != z)
            if window and z in early_zs:
                conds.append(models[dx][0] // 2 + ys[dy] != 0)
            if conds:
                pl.when(functools.reduce(lambda p, q: p & q, conds))(send_one)
            else:
                send_one()
    r_w[pl.ds(chip, 1)] = s_w[...].reshape(1, 9, 2, 128)
    r_x[pl.ds(me, 1)] = s_x[pl.ds(m * N_COLS + c, 1)]

    at_row = m * 16 - 1 + lax.broadcasted_iota(jnp.int32, (10, MID_COL, 128), 1) // 8
    at_col = c * 8 - 1 + lax.broadcasted_iota(jnp.int32, (10, MID_COL, 128), 0)
    inside[...] = jnp.where((at_row >= 0) & (at_row < 128) & (at_col >= 0) & (at_col < 128), 1.0, 0.0)

    def drain(ref, count, sem):
        part = ref.at[pl.ds(0, count)]
        pltpu.make_async_copy(part, part, sem).wait()

    def unpack_w(ref, k):
        for tap in range(9):
            tmp[0, 0:N_DEV] = ref[:, tap].astype(jnp.float32).reshape(N_DEV, 128)
            at = pl.multiple_of(tap * C1 + k * 64, 64)
            for half in range(2):
                w1_mat[pl.ds(at, 64), half * 128 : half * 128 + 128] = tmp.at[0][pl.ds(half, 64, stride=2), :].astype(jnp.bfloat16)

    drain(r_w, 63, recv_w)
    swap = pltpu.make_async_remote_copy(src_ref=r_w, dst_ref=r_w2, send_sem=send_d, recv_sem=recv_d,
                                        device_id=partner, device_id_type=MESH)
    swap.start()
    unpack_w(r_w, core)
    swap.wait_recv()
    unpack_w(r_w2, 1 - core)
    for get in get_b:
        get.wait()
    get_w2.wait()

    drain(r_x, N_DEV - 1, recv_x)
    for half in range(2):
        tmp[half] = r_x[:, half].astype(jnp.float32).reshape(N_DEV * 8, 128)

    def pixels(s):
        return tmp.at[s // 8][pl.ds(s % 8, N_DEV, stride=8), :].T

    for s in range(12, 15):
        edge[s - 12] = pixels(s)
    for w in range(12):
        top = (w % 4) * 32
        col = jnp.concatenate([edge[w // 4, top : top + 16], pixels(w), edge[w // 4, top + 16 : top + 32]])
        xs0[w] = col.astype(jnp.bfloat16)
        xs8[w] = col[8 : 8 + MID_COL].astype(jnp.bfloat16)

    before = None
    for top, rows in ((0, 48), (48, 32), (80, 32), (112, 32)):
        acc = None
        for pair in range(5):
            lhs = []
            for tap in range(2 * pair, min(2 * pair + 2, 9)):
                dh, dw = tap // 3, tap % 3
                src = xs8 if dh == 1 else xs0
                at = top + (16 if dh == 2 else 0)
                lhs.append(src[dw : dw + 10, at : at + rows].reshape(10 * rows, C1))
            lhs = jnp.concatenate(lhs, axis=1) if len(lhs) > 1 else lhs[0]
            term = dot(lhs, w1_mat[pair * 256 : pair * 256 + lhs.shape[1], :])
            acc = term if acc is None else acc + term
        act = jnp.maximum(acc + b1_loc[...], 0.0).reshape(10, rows, C2)
        ok = inside[:, top : top + rows] > 0.0
        real = [jnp.where(ok, act[:, :, half * 128 : half * 128 + 128], 0.0) for half in range(2)]
        for half in range(2):
            part = slice(half * 128, half * 128 + 128)
            ys0[:, top : top + rows, part] = real[half].astype(jnp.bfloat16)
            if before is None:
                ys8[:, 0 : rows - 16, part] = real[half][:, 8 : rows - 8].astype(jnp.bfloat16)
            else:
                shifted = jnp.concatenate([before[half], real[half][:, 0 : rows - 8]], axis=1)
                ys8[:, top - 16 : top + rows - 16, part] = shifted.astype(jnp.bfloat16)
        before = [r[:, rows - 8 :] for r in real]

    for i, (top, rows) in enumerate(BLOCKS):
        conv_two(top, rows, 1, ys0, ys8, w2_mat, b2_loc, res.at[i], out_ref)

    drain(r_w, 63, send_w)
    drain(s_x, N_DEV - 1, send_x)
    swap.wait_send()


def conv_two(top, rows, parts, ys0, ys8, w2_mat, b2_ref, res, out_ref):
    cols = 8 // parts
    size = rows * 8
    for part in range(parts):
        acc = None
        for tap in range(9):
            dh, dw = tap // 3, tap % 3
            src = ys8 if dh == 1 else ys0
            at = top * 8 + (16 if dh == 2 else 0)
            lo = dw + part * cols
            term = dot(src[lo : lo + cols, at : at + size].reshape(cols * size, C2), w2_mat[dh, dw])
            acc = term if acc is None else acc + term
        full = acc + b2_ref[...]
        for w in range(cols):
            for half in range(2):
                to = (part * cols + w) * (size + 8)
                res[half, to : to + size] = full[w * size : w * size + size, half * 128 : half * 128 + 128]
    for h in range(rows):
        for n in range(8):
            for half in range(2):
                vals = res.at[half][pl.ds(h * 8 + n, 8, stride=size + 8), :]
                out_ref[n, top % out_ref.shape[1] + h, :, half * 128 : half * 128 + 128] = vals


def kernel_two(out_a, ys0, ys8, w2_mat, b2_ref, out_hbm, out_b, res, sem):
    put_a = pltpu.make_async_copy(out_a, out_hbm.at[:, 0:LAST], sem.at[0])
    put_a.start()
    conv_two(LAST, 16 - LAST, 1, ys0, ys8, w2_mat, b2_ref, res, out_b)
    put_b = pltpu.make_async_copy(out_b, out_hbm.at[:, LAST:16], sem.at[1])
    put_b.start()
    put_a.wait()
    put_b.wait()


def solution(mesh):
    def run_local(x_in, w_conv1, b_conv1, w_conv2, b_conv2):
        bf, f32 = jnp.bfloat16, jnp.float32
        vmem = pl.BlockSpec(memory_space=pltpu.VMEM)
        hbm = pl.BlockSpec(memory_space=pltpu.HBM)
        dma = pltpu.SemaphoreType.DMA
        operands = (x_in.reshape(x_in.shape[:3]), w_conv1.reshape(3, 3, C2), b_conv1.reshape(1, C2), w_conv2, b_conv2.reshape(1, C2))
        out_a, ys0, ys8, w2 = pl.pallas_call(
            kernel,
            name="conv_pair",
            out_shape=[
                jax.ShapeDtypeStruct((8, LAST, 8, C2), f32),
                jax.ShapeDtypeStruct((10, MID_COL, C2), bf),
                jax.ShapeDtypeStruct((10, 128, C2), bf),
                jax.ShapeDtypeStruct((3, 3, C2, C2), bf),
            ],
            in_specs=[hbm] * 5,
            out_specs=[vmem] * 4,
            scratch_shapes=[
                pltpu.VMEM((8, 128, 128), bf),
                pltpu.VMEM((3, 3, C2), bf),
                pltpu.VMEM((1, C2), f32),
                pltpu.VMEM((1, C2), f32),
                pltpu.VMEM((128, 1024), bf),
                pltpu.VMEM((1024, 2048), bf),
                pltpu.VMEM((256, 1024), bf),
                pltpu.VMEM((256, 256), bf),
                pltpu.VMEM((9, 2, 128), bf),
                pltpu.VMEM((N_DEV, 2, 8, 128), bf),
                pltpu.VMEM((64, 9, 2, 128), bf),
                pltpu.VMEM((64, 9, 2, 128), bf),
                pltpu.VMEM((N_DEV, 2, 8, 128), bf),
                pltpu.VMEM((9 * C1, C2), bf),
                pltpu.VMEM((2, N_DEV * 8, 128), f32),
                pltpu.VMEM((3, 128, 128), f32),
                pltpu.VMEM((12, COL, C1), bf),
                pltpu.VMEM((12, MID_COL, C1), bf),
                pltpu.VMEM((10, MID_COL, 128), f32),
                pltpu.VMEM((len(BLOCKS), 2, 8 * OUT_COL, 128), f32),
                pltpu.SemaphoreType.REGULAR, dma, dma, pltpu.SemaphoreType.DMA((2,)), dma,
                dma, dma, dma, dma, dma, dma,
            ],
            compiler_params=pltpu.CompilerParams(collective_id=0, has_side_effects=True, vmem_limit_bytes=24 << 20),
        )(*(pltpu.with_memory_space_constraint(a, pltpu.HBM) for a in operands))
        return pl.pallas_call(
            kernel_two,
            name="conv_last",
            out_shape=jax.ShapeDtypeStruct((8, 16, 8, C2), f32),
            in_specs=[vmem] * 5,
            out_specs=hbm,
            scratch_shapes=[pltpu.VMEM((8, 16 - LAST, 8, C2), f32), pltpu.VMEM((2, 8 * OUT_COL, 128), f32), pltpu.SemaphoreType.DMA((2,))],
            compiler_params=pltpu.CompilerParams(vmem_limit_bytes=24 << 20),
        )(out_a, ys0, ys8, w2, operands[-1])

    return jax.shard_map(
        run_local,
        mesh=mesh,
        in_specs=(P("data", None, None, GROUP_AXES), P(None, None, GROUP_AXES, None), P(), P(), P()),
        out_specs=P("data", "model", "cols", None),
        check_vma=False,
    )
```

```python
import collections
import functools

import jax
import jax.numpy as jnp
from jax import lax
from jax.experimental import pallas as pl
from jax.experimental.pallas import tpu as pltpu
from jax.sharding import PartitionSpec as P

MESH = pl.DeviceIdType.MESH
GROUP_AXES = ("model", "cols")

N_DEV = 128
N_COLS = 16
COL = 160
MID_COL = 144
OUT_COL = 40
BLOCKS = ((0, 4), (4, 4), (8, 4), (12, 2))
LAST = 14
C1 = 128
C2 = 256
HOPS = (0, 1, 2, 1)


def greet_order():
    shifts = [(dx, dy, dz) for dx in range(4) for dy in range(4) for dz in range(4)][1:]
    return sorted(shifts, key=lambda s: (-HOPS[s[1]] - HOPS[s[2]], -HOPS[s[0]]))


GREET_ORDER = greet_order()
LATER_Z = ((0, 6, 14, 11), (100, 100, 108, 105))
LATER_Y = ((20, 6, 0, 10), (20, 8, 0, 12))
LATER_X = ((-3, 0, -1, -2), (0.0, 0.31000000000000005, 0.30000000000000004, 0.1))
LATER_CORE = -0.01
MIX = (0, 1, 1, 1, 1, 1)
EARLY = (1,)


def send_order():
    def key(msg):
        window, dx, dy, z, dk = msg
        mix = (MIX[1] * window + MIX[2] * dx + MIX[3] * dy + MIX[4] * z) * (MIX[5] + dk) % 17
        return LATER_Z[window][z] + LATER_Y[window][dy] + LATER_X[window][dx] + LATER_CORE * dk + MIX[0] * mix

    windows = [(1, dx, dy, z, dk) for dx in range(4) for dy in range(4) for z in range(4) for dk in range(2)]
    weights = [(0, dx, dy, z, 0) for dx in range(4) for dy in range(4) for z in range(4)]
    order = sorted(weights + windows, key=key)
    return [m for m in order if m[3] == 0], [m for m in order if m[3] > 0]


SEND_ORDER = send_order()


def dot(a, b):
    return lax.dot_general(a, b, (((1,), (0,)), ((), ())), preferred_element_type=jnp.float32)


def kernel(x_hbm, w1_hbm, b1_hbm, w2_hbm, b2_hbm, out_ref, ys0, ys8, w2_mat,
           x_loc, w1_loc, b1_loc, b2_loc, turned, pick, sel, place, s_w, s_x, r_w, r_w2, r_x,
           w1_mat, tmp, edge, xs0, xs8, inside, res,
           heard, sem_x, sem_w1, sem_b, sem_w2, send_w, send_x, send_d, recv_w, recv_x, recv_d):
    m = lax.axis_index("model")
    c = lax.axis_index("cols")
    core = m % 2
    chip = m // 2 * N_COLS + c
    me = core * 64 + chip

    get_x = pltpu.make_async_copy(x_hbm, x_loc, sem_x)
    get_x.start()
    get_w1 = pltpu.make_async_copy(w1_hbm, w1_loc, sem_w1)
    get_w1.start()
    get_b = (pltpu.make_async_copy(b1_hbm, b1_loc, sem_b.at[0]), pltpu.make_async_copy(b2_hbm, b2_loc, sem_b.at[1]))
    for get in get_b:
        get.start()
    get_w2 = pltpu.make_async_copy(w2_hbm, w2_mat, sem_w2)
    get_w2.start()

    cores = (core, 1 - core)
    models = [[((m // 2 + dx) % 4) * 2 + k for k in cores] for dx in range(4)]
    ys = [(c % 4 + dy) % 4 for dy in range(4)]
    my_z = c // 4
    zs = [((my_z + dz) % 4) * 4 for dz in range(4)]

    barrier = pltpu.get_barrier_semaphore()
    part = (my_z + 3) // 4
    partner = {"model": m + 1 - 2 * core, "cols": c}
    for dx, dy, dz in GREET_ORDER:
        to = {"model": ((m // 2 + dx) % 4) * 2 + part, "cols": zs[dz] + ys[dy]}
        pl.semaphore_signal(barrier, inc=1, device_id=to, device_id_type=MESH)
    pl.semaphore_signal(barrier, inc=1, device_id=partner, device_id_type=MESH)

    def hear(which):
        @pl.when(core == which)
        def _():
            pl.semaphore_wait(barrier, (32, 96)[which] - 1 + 2 * ((core + part) % 2))
            pl.semaphore_signal(heard, inc=1, device_id=partner, device_id_type=MESH)

        @pl.when(core != which)
        def _():
            pl.semaphore_wait(heard, 1)

    for blk in range(4):
        lane = blk * 512 + lax.broadcasted_iota(jnp.int32, (1, 512), 1)
        img = lane % 8
        if blk < 2:
            row = (lane // 128) * 16 + (lane // 8) % 16
        else:
            h = (lane // 8) % 4
            row = (lane // 128 - 8) * 16 + h - 2 + jnp.where(h >= 2, 16, 0)
        at = jnp.where((row >= 0) & (row < 128), img * 128 + row, -1)
        for pair in range(4):
            rows = pair * 256 + lax.broadcasted_iota(jnp.int32, (256, 512), 0)
            pick[pair * 256 : pair * 256 + 256, blk * 512 : blk * 512 + 512] = jnp.where(rows == at, 1.0, 0.0).astype(jnp.bfloat16)
    r_id = lax.broadcasted_iota(jnp.int32, (256, 256), 0)
    k_id = lax.broadcasted_iota(jnp.int32, (256, 256), 1)
    first = (r_id // 16) * 8 - 2
    s_id = r_id % 16
    main = (s_id < 12) & (k_id == first + s_id) & (k_id < 128)
    from_col = first + 4 * (s_id - 12)
    border = (s_id >= 12) & (s_id < 15) & (k_id >= 128 + jnp.maximum(from_col, 0)) & (k_id < 132 + from_col)
    place[...] = jnp.where(main | border, 1.0, 0.0).astype(jnp.bfloat16)
    get_w1.wait()
    for tap in range(9):
        s_w[tap] = jnp.concatenate([w1_loc[tap // 3, tap % 3 : tap % 3 + 1, half * 128 : half * 128 + 128] for half in range(2)])

    get_x.wait()
    for n in range(8):
        turned[:, n * 128 : n * 128 + 128] = x_loc[n].T
    w_id = lax.broadcasted_iota(jnp.int32, (128, 256), 0)
    l_id = lax.broadcasted_iota(jnp.int32, (128, 256), 1) % 128
    keep = (l_id // 32) == ((w_id + 2) % 4)
    for blk in range(8):
        z = None
        for pair in range(4):
            term = dot(turned[:, pair * 256 : pair * 256 + 256], pick[pair * 256 : pair * 256 + 256, blk * 256 : blk * 256 + 256])
            z = term if z is None else z + term
        if blk >= 4:
            z = jnp.where(keep, z, 0.0)
        top = 0 if blk < 4 else 128
        sel[top : top + 128, (blk % 4) * 256 : (blk % 4) * 256 + 256] = z.astype(jnp.bfloat16)
    for blk in range(4):
        t = dot(place[...], sel[:, blk * 256 : blk * 256 + 256])
        for r in range(2):
            tiles = t[:, r * 128 : r * 128 + 128].reshape(16, 2, 8, 128).astype(jnp.bfloat16)
            s_x[(blk * 2 + r) * 16 : (blk * 2 + r) * 16 + 16] = tiles


    def send(src, dst, send_sem, recv_sem, pm, pc):
        pltpu.make_async_remote_copy(src_ref=src, dst_ref=dst, send_sem=send_sem, recv_sem=recv_sem,
                                     device_id={"model": pm, "cols": pc}, device_id_type=MESH).start()

    for which, order in enumerate(SEND_ORDER):
        hear(which)
        served = set()
        for window, dx, dy, z, dk in order:
            if window and z in EARLY and z not in served:
                served.add(z)
                for k in (1, 0):
                    def send_early(pm=k, pc=z * 4):
                        send(s_x.at[pm * N_COLS + pc], r_x.at[me], send_x, recv_x, pm, pc)
                    pl.when((m != k) | (c != z * 4))(send_early)
            pm, pc = models[dx][dk], z * 4 + ys[dy]

            def send_one(window=window, pm=pm, pc=pc):
                if window:
                    send(s_x.at[pm * N_COLS + pc], r_x.at[me], send_x, recv_x, pm, pc)
                else:
                    send(s_w, r_w.at[chip], send_w, recv_w, pm, pc)

            conds = []
            if dx == dy == dk == 0:
                conds.append(my_z != z)
            if window and z in EARLY:
                conds.append(models[dx][0] // 2 + ys[dy] != 0)
            if conds:
                pl.when(functools.reduce(lambda p, q: p & q, conds))(send_one)
            else:
                send_one()
    r_w[pl.ds(chip, 1)] = s_w[...].reshape(1, 9, 2, 128)
    r_x[pl.ds(me, 1)] = s_x[pl.ds(m * N_COLS + c, 1)]

    at_row = m * 16 - 1 + lax.broadcasted_iota(jnp.int32, (10, MID_COL, 128), 1) // 8
    at_col = c * 8 - 1 + lax.broadcasted_iota(jnp.int32, (10, MID_COL, 128), 0)
    inside[...] = jnp.where((at_row >= 0) & (at_row < 128) & (at_col >= 0) & (at_col < 128), 1.0, 0.0)

    def drain(ref, count, sem):
        part = ref.at[pl.ds(0, count)]
        pltpu.make_async_copy(part, part, sem).wait()

    def unpack_w(ref, k):
        for tap in range(9):
            tmp[0, 0:N_DEV] = ref[:, tap].astype(jnp.float32).reshape(N_DEV, 128)
            at = pl.multiple_of(tap * C1 + k * 64, 64)
            for half in range(2):
                w1_mat[pl.ds(at, 64), half * 128 : half * 128 + 128] = tmp.at[0][pl.ds(half, 64, stride=2), :].astype(jnp.bfloat16)

    drain(r_w, 63, recv_w)
    swap = pltpu.make_async_remote_copy(src_ref=r_w, dst_ref=r_w2, send_sem=send_d, recv_sem=recv_d,
                                        device_id=partner, device_id_type=MESH)
    swap.start()
    unpack_w(r_w, core)
    swap.wait_recv()
    unpack_w(r_w2, 1 - core)
    for get in get_b:
        get.wait()
    get_w2.wait()

    drain(r_x, N_DEV - 1, recv_x)
    for half in range(2):
        tmp[half] = r_x[:, half].astype(jnp.float32).reshape(N_DEV * 8, 128)

    def pixels(s):
        return tmp.at[s // 8][pl.ds(s % 8, N_DEV, stride=8), :].T

    for s in range(12, 15):
        edge[s - 12] = pixels(s)
    for w in range(12):
        top = (w % 4) * 32
        col = jnp.concatenate([edge[w // 4, top : top + 16], pixels(w), edge[w // 4, top + 16 : top + 32]])
        xs0[w] = col.astype(jnp.bfloat16)
        xs8[w] = col[8 : 8 + MID_COL].astype(jnp.bfloat16)

    before = None
    for top, rows in ((0, 48), (48, 32), (80, 32), (112, 32)):
        acc = None
        for pair in range(5):
            lhs = []
            for tap in range(2 * pair, min(2 * pair + 2, 9)):
                dh, dw = tap // 3, tap % 3
                src = xs8 if dh == 1 else xs0
                at = top + (16 if dh == 2 else 0)
                lhs.append(src[dw : dw + 10, at : at + rows].reshape(10 * rows, C1))
            lhs = jnp.concatenate(lhs, axis=1) if len(lhs) > 1 else lhs[0]
            term = dot(lhs, w1_mat[pair * 256 : pair * 256 + lhs.shape[1], :])
            acc = term if acc is None else acc + term
        act = jnp.maximum(acc + b1_loc[...], 0.0).reshape(10, rows, C2)
        ok = inside[:, top : top + rows] > 0.0
        real = [jnp.where(ok, act[:, :, half * 128 : half * 128 + 128], 0.0) for half in range(2)]
        for half in range(2):
            part = slice(half * 128, half * 128 + 128)
            ys0[:, top : top + rows, part] = real[half].astype(jnp.bfloat16)
            if before is None:
                ys8[:, 0 : rows - 16, part] = real[half][:, 8 : rows - 8].astype(jnp.bfloat16)
            else:
                shifted = jnp.concatenate([before[half], real[half][:, 0 : rows - 8]], axis=1)
                ys8[:, top - 16 : top + rows - 16, part] = shifted.astype(jnp.bfloat16)
        before = [r[:, rows - 8 :] for r in real]

    for i, (top, rows) in enumerate(BLOCKS):
        conv_two(top, rows, 1, ys0, ys8, w2_mat, b2_loc, res.at[i], out_ref)

    drain(r_w, 63, send_w)
    drain(s_x, N_DEV - 1, send_x)
    swap.wait_send()


def conv_two(top, rows, parts, ys0, ys8, w2_mat, b2_ref, res, out_ref):
    cols = 8 // parts
    size = rows * 8
    for part in range(parts):
        acc = None
        for tap in range(9):
            dh, dw = tap // 3, tap % 3
            src = ys8 if dh == 1 else ys0
            at = top * 8 + (16 if dh == 2 else 0)
            lo = dw + part * cols
            term = dot(src[lo : lo + cols, at : at + size].reshape(cols * size, C2), w2_mat[dh, dw])
            acc = term if acc is None else acc + term
        full = acc + b2_ref[...]
        for w in range(cols):
            for half in range(2):
                to = (part * cols + w) * (size + 8)
                res[half, to : to + size] = full[w * size : w * size + size, half * 128 : half * 128 + 128]
    for h in range(rows):
        for n in range(8):
            for half in range(2):
                vals = res.at[half][pl.ds(h * 8 + n, 8, stride=size + 8), :]
                out_ref[n, top % out_ref.shape[1] + h, :, half * 128 : half * 128 + 128] = vals


def kernel_two(out_a, ys0, ys8, w2_mat, b2_ref, out_hbm, out_b, res, sem):
    put_a = pltpu.make_async_copy(out_a, out_hbm.at[:, 0:LAST], sem.at[0])
    put_a.start()
    conv_two(LAST, 16 - LAST, 1, ys0, ys8, w2_mat, b2_ref, res, out_b)
    put_b = pltpu.make_async_copy(out_b, out_hbm.at[:, LAST:16], sem.at[1])
    put_b.start()
    put_a.wait()
    put_b.wait()


def solution(mesh):
    def run_local(x_in, w_conv1, b_conv1, w_conv2, b_conv2):
        bf, f32 = jnp.bfloat16, jnp.float32
        vmem = pl.BlockSpec(memory_space=pltpu.VMEM)
        hbm = pl.BlockSpec(memory_space=pltpu.HBM)
        dma = pltpu.SemaphoreType.DMA
        operands = (x_in.reshape(x_in.shape[:3]), w_conv1.reshape(3, 3, C2), b_conv1.reshape(1, C2), w_conv2, b_conv2.reshape(1, C2))
        out_a, ys0, ys8, w2 = pl.pallas_call(
            kernel,
            name="conv_pair",
            out_shape=[
                jax.ShapeDtypeStruct((8, LAST, 8, C2), f32),
                jax.ShapeDtypeStruct((10, MID_COL, C2), bf),
                jax.ShapeDtypeStruct((10, 128, C2), bf),
                jax.ShapeDtypeStruct((3, 3, C2, C2), bf),
            ],
            in_specs=[hbm] * 5,
            out_specs=[vmem] * 4,
            scratch_shapes=[
                pltpu.VMEM((8, 128, 128), bf),
                pltpu.VMEM((3, 3, C2), bf),
                pltpu.VMEM((1, C2), f32),
                pltpu.VMEM((1, C2), f32),
                pltpu.VMEM((128, 1024), bf),
                pltpu.VMEM((1024, 2048), bf),
                pltpu.VMEM((256, 1024), bf),
                pltpu.VMEM((256, 256), bf),
                pltpu.VMEM((9, 2, 128), bf),
                pltpu.VMEM((N_DEV, 2, 8, 128), bf),
                pltpu.VMEM((64, 9, 2, 128), bf),
                pltpu.VMEM((64, 9, 2, 128), bf),
                pltpu.VMEM((N_DEV, 2, 8, 128), bf),
                pltpu.VMEM((9 * C1, C2), bf),
                pltpu.VMEM((2, N_DEV * 8, 128), f32),
                pltpu.VMEM((3, 128, 128), f32),
                pltpu.VMEM((12, COL, C1), bf),
                pltpu.VMEM((12, MID_COL, C1), bf),
                pltpu.VMEM((10, MID_COL, 128), f32),
                pltpu.VMEM((len(BLOCKS), 2, 8 * OUT_COL, 128), f32),
                pltpu.SemaphoreType.REGULAR, dma, dma, pltpu.SemaphoreType.DMA((2,)), dma,
                dma, dma, dma, dma, dma, dma,
            ],
            compiler_params=pltpu.CompilerParams(collective_id=0, has_side_effects=True, vmem_limit_bytes=24 << 20),
        )(*(pltpu.with_memory_space_constraint(a, pltpu.HBM) for a in operands))
        return pl.pallas_call(
            kernel_two,
            name="conv_last",
            out_shape=jax.ShapeDtypeStruct((8, 16, 8, C2), f32),
            in_specs=[vmem] * 5,
            out_specs=hbm,
            scratch_shapes=[pltpu.VMEM((8, 16 - LAST, 8, C2), f32), pltpu.VMEM((2, 8 * OUT_COL, 128), f32), pltpu.SemaphoreType.DMA((2,))],
            compiler_params=pltpu.CompilerParams(vmem_limit_bytes=24 << 20),
        )(out_a, ys0, ys8, w2, operands[-1])

    return jax.shard_map(
        run_local,
        mesh=mesh,
        in_specs=(P("data", None, None, GROUP_AXES), P(None, None, GROUP_AXES, None), P(), P(), P()),
        out_specs=P("data", "model", "cols", None),
        check_vma=False,
    )
```

```python
import collections
import functools

import jax
import jax.numpy as jnp
from jax import lax
from jax.experimental import pallas as pl
from jax.experimental.pallas import tpu as pltpu
from jax.sharding import PartitionSpec as P

MESH = pl.DeviceIdType.MESH
GROUP_AXES = ("model", "cols")

N_DEV = 128
N_COLS = 16
COL = 160
MID_COL = 144
OUT_COL = 40
BLOCKS = ((0, 4), (4, 4), (8, 4), (12, 2))
LAST = 14
C1 = 128
C2 = 256
HOPS = (0, 1, 2, 1)


def greet_order():
    shifts = [(dx, dy, dz) for dx in range(4) for dy in range(4) for dz in range(4)][1:]
    return sorted(shifts, key=lambda s: (-HOPS[s[1]] - HOPS[s[2]], -HOPS[s[0]]))


GREET_ORDER = greet_order()
LATER_Z = ((0, 3, 17, 11), (100, 100, 108, 105))
LATER_Y = ((20, 6, 0, 12), (17, 8, 0, 12))
LATER_X = ((-6, 0, -1, -2), (0.0, 0.31, 0.3, 0.1))
LATER_CORE = 0.01
MIX = (0, 1, 1, 1, 1, 1)
EARLY = (1, 2)


def send_order():
    def key(msg):
        window, dx, dy, z, dk = msg
        mix = (MIX[1] * window + MIX[2] * dx + MIX[3] * dy + MIX[4] * z) * (MIX[5] + dk) % 17
        return LATER_Z[window][z] + LATER_Y[window][dy] + LATER_X[window][dx] + LATER_CORE * dk + MIX[0] * mix

    windows = [(1, dx, dy, z, dk) for dx in range(4) for dy in range(4) for z in range(4) for dk in range(2)]
    weights = [(0, dx, dy, z, 0) for dx in range(4) for dy in range(4) for z in range(4)]
    order = sorted(weights + windows, key=key)
    return [m for m in order if m[3] == 0], [m for m in order if m[3] > 0]


SEND_ORDER = send_order()


def dot(a, b):
    return lax.dot_general(a, b, (((1,), (0,)), ((), ())), preferred_element_type=jnp.float32)


def kernel(x_hbm, w1_hbm, b1_hbm, w2_hbm, b2_hbm, out_ref, ys0, ys8, w2_mat,
           x_loc, w1_loc, b1_loc, b2_loc, turned, pick, sel, place, s_w, s_x, r_w, r_w2, r_x,
           w1_mat, tmp, edge, xs0, xs8, inside, res,
           heard, sem_x, sem_w1, sem_b, sem_w2, send_w, send_x, send_d, recv_w, recv_x, recv_d):
    m = lax.axis_index("model")
    c = lax.axis_index("cols")
    core = m % 2
    chip = m // 2 * N_COLS + c
    me = core * 64 + chip

    get_x = pltpu.make_async_copy(x_hbm, x_loc, sem_x)
    get_x.start()
    get_w1 = pltpu.make_async_copy(w1_hbm, w1_loc, sem_w1)
    get_w1.start()
    get_b = (pltpu.make_async_copy(b1_hbm, b1_loc, sem_b.at[0]), pltpu.make_async_copy(b2_hbm, b2_loc, sem_b.at[1]))
    for get in get_b:
        get.start()
    get_w2 = pltpu.make_async_copy(w2_hbm, w2_mat, sem_w2)
    get_w2.start()

    cores = (core, 1 - core)
    models = [[((m // 2 + dx) % 4) * 2 + k for k in cores] for dx in range(4)]
    ys = [(c % 4 + dy) % 4 for dy in range(4)]
    my_z = c // 4
    zs = [((my_z + dz) % 4) * 4 for dz in range(4)]

    barrier = pltpu.get_barrier_semaphore()
    part = (my_z + 3) // 4
    partner = {"model": m + 1 - 2 * core, "cols": c}
    for dx, dy, dz in GREET_ORDER:
        to = {"model": ((m // 2 + dx) % 4) * 2 + part, "cols": zs[dz] + ys[dy]}
        pl.semaphore_signal(barrier, inc=1, device_id=to, device_id_type=MESH)
    pl.semaphore_signal(barrier, inc=1, device_id=partner, device_id_type=MESH)

    def hear(which):
        @pl.when(core == which)
        def _():
            pl.semaphore_wait(barrier, (32, 96)[which] - 1 + 2 * ((core + part) % 2))
            pl.semaphore_signal(heard, inc=1, device_id=partner, device_id_type=MESH)

        @pl.when(core != which)
        def _():
            pl.semaphore_wait(heard, 1)

    for blk in range(4):
        lane = blk * 512 + lax.broadcasted_iota(jnp.int32, (1, 512), 1)
        img = lane % 8
        if blk < 2:
            row = (lane // 128) * 16 + (lane // 8) % 16
        else:
            h = (lane // 8) % 4
            row = (lane // 128 - 8) * 16 + h - 2 + jnp.where(h >= 2, 16, 0)
        at = jnp.where((row >= 0) & (row < 128), img * 128 + row, -1)
        for pair in range(4):
            rows = pair * 256 + lax.broadcasted_iota(jnp.int32, (256, 512), 0)
            pick[pair * 256 : pair * 256 + 256, blk * 512 : blk * 512 + 512] = jnp.where(rows == at, 1.0, 0.0).astype(jnp.bfloat16)
    r_id = lax.broadcasted_iota(jnp.int32, (256, 256), 0)
    k_id = lax.broadcasted_iota(jnp.int32, (256, 256), 1)
    first = (r_id // 16) * 8 - 2
    s_id = r_id % 16
    main = (s_id < 12) & (k_id == first + s_id) & (k_id < 128)
    from_col = first + 4 * (s_id - 12)
    border = (s_id >= 12) & (s_id < 15) & (k_id >= 128 + jnp.maximum(from_col, 0)) & (k_id < 132 + from_col)
    place[...] = jnp.where(main | border, 1.0, 0.0).astype(jnp.bfloat16)
    get_w1.wait()
    for tap in range(9):
        s_w[tap] = jnp.concatenate([w1_loc[tap // 3, tap % 3 : tap % 3 + 1, half * 128 : half * 128 + 128] for half in range(2)])

    get_x.wait()
    for n in range(8):
        turned[:, n * 128 : n * 128 + 128] = x_loc[n].T
    w_id = lax.broadcasted_iota(jnp.int32, (128, 256), 0)
    l_id = lax.broadcasted_iota(jnp.int32, (128, 256), 1) % 128
    keep = (l_id // 32) == ((w_id + 2) % 4)
    for blk in range(8):
        z = None
        for pair in range(4):
            term = dot(turned[:, pair * 256 : pair * 256 + 256], pick[pair * 256 : pair * 256 + 256, blk * 256 : blk * 256 + 256])
            z = term if z is None else z + term
        if blk >= 4:
            z = jnp.where(keep, z, 0.0)
        top = 0 if blk < 4 else 128
        sel[top : top + 128, (blk % 4) * 256 : (blk % 4) * 256 + 256] = z.astype(jnp.bfloat16)
    for blk in range(4):
        t = dot(place[...], sel[:, blk * 256 : blk * 256 + 256])
        for r in range(2):
            tiles = t[:, r * 128 : r * 128 + 128].reshape(16, 2, 8, 128).astype(jnp.bfloat16)
            s_x[(blk * 2 + r) * 16 : (blk * 2 + r) * 16 + 16] = tiles


    def send(src, dst, send_sem, recv_sem, pm, pc):
        pltpu.make_async_remote_copy(src_ref=src, dst_ref=dst, send_sem=send_sem, recv_sem=recv_sem,
                                     device_id={"model": pm, "cols": pc}, device_id_type=MESH).start()

    for which, order in enumerate(SEND_ORDER):
        hear(which)
        served = set()
        for window, dx, dy, z, dk in order:
            if window and z in EARLY and z not in served:
                served.add(z)
                for k in (1, 0):
                    def send_early(pm=k, pc=z * 4):
                        send(s_x.at[pm * N_COLS + pc], r_x.at[me], send_x, recv_x, pm, pc)
                    pl.when((m != k) | (c != z * 4))(send_early)
            pm, pc = models[dx][dk], z * 4 + ys[dy]

            def send_one(window=window, pm=pm, pc=pc):
                if window:
                    send(s_x.at[pm * N_COLS + pc], r_x.at[me], send_x, recv_x, pm, pc)
                else:
                    send(s_w, r_w.at[chip], send_w, recv_w, pm, pc)

            conds = []
            if dx == dy == dk == 0:
                conds.append(my_z != z)
            if window and z in EARLY:
                conds.append(models[dx][0] // 2 + ys[dy] != 0)
            if conds:
                pl.when(functools.reduce(lambda p, q: p & q, conds))(send_one)
            else:
                send_one()
    r_w[pl.ds(chip, 1)] = s_w[...].reshape(1, 9, 2, 128)
    r_x[pl.ds(me, 1)] = s_x[pl.ds(m * N_COLS + c, 1)]

    at_row = m * 16 - 1 + lax.broadcasted_iota(jnp.int32, (10, MID_COL, 128), 1) // 8
    at_col = c * 8 - 1 + lax.broadcasted_iota(jnp.int32, (10, MID_COL, 128), 0)
    inside[...] = jnp.where((at_row >= 0) & (at_row < 128) & (at_col >= 0) & (at_col < 128), 1.0, 0.0)

    def drain(ref, count, sem):
        part = ref.at[pl.ds(0, count)]
        pltpu.make_async_copy(part, part, sem).wait()

    def unpack_w(ref, k):
        for tap in range(9):
            tmp[0, 0:N_DEV] = ref[:, tap].astype(jnp.float32).reshape(N_DEV, 128)
            at = pl.multiple_of(tap * C1 + k * 64, 64)
            for half in range(2):
                w1_mat[pl.ds(at, 64), half * 128 : half * 128 + 128] = tmp.at[0][pl.ds(half, 64, stride=2), :].astype(jnp.bfloat16)

    drain(r_w, 63, recv_w)
    swap = pltpu.make_async_remote_copy(src_ref=r_w, dst_ref=r_w2, send_sem=send_d, recv_sem=recv_d,
                                        device_id=partner, device_id_type=MESH)
    swap.start()
    unpack_w(r_w, core)
    swap.wait_recv()
    unpack_w(r_w2, 1 - core)
    for get in get_b:
        get.wait()
    get_w2.wait()

    drain(r_x, N_DEV - 1, recv_x)
    for half in range(2):
        tmp[half] = r_x[:, half].astype(jnp.float32).reshape(N_DEV * 8, 128)

    def pixels(s):
        return tmp.at[s // 8][pl.ds(s % 8, N_DEV, stride=8), :].T

    for s in range(12, 15):
        edge[s - 12] = pixels(s)
    for w in range(12):
        top = (w % 4) * 32
        col = jnp.concatenate([edge[w // 4, top : top + 16], pixels(w), edge[w // 4, top + 16 : top + 32]])
        xs0[w] = col.astype(jnp.bfloat16)
        xs8[w] = col[8 : 8 + MID_COL].astype(jnp.bfloat16)

    before = None
    for top, rows in ((0, 48), (48, 32), (80, 32), (112, 32)):
        acc = None
        for pair in range(5):
            lhs = []
            for tap in range(2 * pair, min(2 * pair + 2, 9)):
                dh, dw = tap // 3, tap % 3
                src = xs8 if dh == 1 else xs0
                at = top + (16 if dh == 2 else 0)
                lhs.append(src[dw : dw + 10, at : at + rows].reshape(10 * rows, C1))
            lhs = jnp.concatenate(lhs, axis=1) if len(lhs) > 1 else lhs[0]
            term = dot(lhs, w1_mat[pair * 256 : pair * 256 + lhs.shape[1], :])
            acc = term if acc is None else acc + term
        act = jnp.maximum(acc + b1_loc[...], 0.0).reshape(10, rows, C2)
        ok = inside[:, top : top + rows] > 0.0
        real = [jnp.where(ok, act[:, :, half * 128 : half * 128 + 128], 0.0) for half in range(2)]
        for half in range(2):
            part = slice(half * 128, half * 128 + 128)
            ys0[:, top : top + rows, part] = real[half].astype(jnp.bfloat16)
            if before is None:
                ys8[:, 0 : rows - 16, part] = real[half][:, 8 : rows - 8].astype(jnp.bfloat16)
            else:
                shifted = jnp.concatenate([before[half], real[half][:, 0 : rows - 8]], axis=1)
                ys8[:, top - 16 : top + rows - 16, part] = shifted.astype(jnp.bfloat16)
        before = [r[:, rows - 8 :] for r in real]

    for i, (top, rows) in enumerate(BLOCKS):
        conv_two(top, rows, 1, ys0, ys8, w2_mat, b2_loc, res.at[i], out_ref)

    drain(r_w, 63, send_w)
    drain(s_x, N_DEV - 1, send_x)
    swap.wait_send()


def conv_two(top, rows, parts, ys0, ys8, w2_mat, b2_ref, res, out_ref):
    cols = 8 // parts
    size = rows * 8
    for part in range(parts):
        acc = None
        for tap in range(9):
            dh, dw = tap // 3, tap % 3
            src = ys8 if dh == 1 else ys0
            at = top * 8 + (16 if dh == 2 else 0)
            lo = dw + part * cols
            term = dot(src[lo : lo + cols, at : at + size].reshape(cols * size, C2), w2_mat[dh, dw])
            acc = term if acc is None else acc + term
        full = acc + b2_ref[...]
        for w in range(cols):
            for half in range(2):
                to = (part * cols + w) * (size + 8)
                res[half, to : to + size] = full[w * size : w * size + size, half * 128 : half * 128 + 128]
    for h in range(rows):
        for n in range(8):
            for half in range(2):
                vals = res.at[half][pl.ds(h * 8 + n, 8, stride=size + 8), :]
                out_ref[n, top % out_ref.shape[1] + h, :, half * 128 : half * 128 + 128] = vals


def kernel_two(out_a, ys0, ys8, w2_mat, b2_ref, out_hbm, out_b, res, sem):
    put_a = pltpu.make_async_copy(out_a, out_hbm.at[:, 0:LAST], sem.at[0])
    put_a.start()
    conv_two(LAST, 16 - LAST, 1, ys0, ys8, w2_mat, b2_ref, res, out_b)
    put_b = pltpu.make_async_copy(out_b, out_hbm.at[:, LAST:16], sem.at[1])
    put_b.start()
    put_a.wait()
    put_b.wait()


def solution(mesh):
    def run_local(x_in, w_conv1, b_conv1, w_conv2, b_conv2):
        bf, f32 = jnp.bfloat16, jnp.float32
        vmem = pl.BlockSpec(memory_space=pltpu.VMEM)
        hbm = pl.BlockSpec(memory_space=pltpu.HBM)
        dma = pltpu.SemaphoreType.DMA
        operands = (x_in.reshape(x_in.shape[:3]), w_conv1.reshape(3, 3, C2), b_conv1.reshape(1, C2), w_conv2, b_conv2.reshape(1, C2))
        out_a, ys0, ys8, w2 = pl.pallas_call(
            kernel,
            name="conv_pair",
            out_shape=[
                jax.ShapeDtypeStruct((8, LAST, 8, C2), f32),
                jax.ShapeDtypeStruct((10, MID_COL, C2), bf),
                jax.ShapeDtypeStruct((10, 128, C2), bf),
                jax.ShapeDtypeStruct((3, 3, C2, C2), bf),
            ],
            in_specs=[hbm] * 5,
            out_specs=[vmem] * 4,
            scratch_shapes=[
                pltpu.VMEM((8, 128, 128), bf),
                pltpu.VMEM((3, 3, C2), bf),
                pltpu.VMEM((1, C2), f32),
                pltpu.VMEM((1, C2), f32),
                pltpu.VMEM((128, 1024), bf),
                pltpu.VMEM((1024, 2048), bf),
                pltpu.VMEM((256, 1024), bf),
                pltpu.VMEM((256, 256), bf),
                pltpu.VMEM((9, 2, 128), bf),
                pltpu.VMEM((N_DEV, 2, 8, 128), bf),
                pltpu.VMEM((64, 9, 2, 128), bf),
                pltpu.VMEM((64, 9, 2, 128), bf),
                pltpu.VMEM((N_DEV, 2, 8, 128), bf),
                pltpu.VMEM((9 * C1, C2), bf),
                pltpu.VMEM((2, N_DEV * 8, 128), f32),
                pltpu.VMEM((3, 128, 128), f32),
                pltpu.VMEM((12, COL, C1), bf),
                pltpu.VMEM((12, MID_COL, C1), bf),
                pltpu.VMEM((10, MID_COL, 128), f32),
                pltpu.VMEM((len(BLOCKS), 2, 8 * OUT_COL, 128), f32),
                pltpu.SemaphoreType.REGULAR, dma, dma, pltpu.SemaphoreType.DMA((2,)), dma,
                dma, dma, dma, dma, dma, dma,
            ],
            compiler_params=pltpu.CompilerParams(collective_id=0, has_side_effects=True, vmem_limit_bytes=24 << 20),
        )(*(pltpu.with_memory_space_constraint(a, pltpu.HBM) for a in operands))
        return pl.pallas_call(
            kernel_two,
            name="conv_last",
            out_shape=jax.ShapeDtypeStruct((8, 16, 8, C2), f32),
            in_specs=[vmem] * 5,
            out_specs=hbm,
            scratch_shapes=[pltpu.VMEM((8, 16 - LAST, 8, C2), f32), pltpu.VMEM((2, 8 * OUT_COL, 128), f32), pltpu.SemaphoreType.DMA((2,))],
            compiler_params=pltpu.CompilerParams(vmem_limit_bytes=24 << 20),
        )(out_a, ys0, ys8, w2, operands[-1])

    return jax.shard_map(
        run_local,
        mesh=mesh,
        in_specs=(P("data", None, None, GROUP_AXES), P(None, None, GROUP_AXES, None), P(), P(), P()),
        out_specs=P("data", "model", "cols", None),
        check_vma=False,
    )
```

```python
import collections
import functools

import jax
import jax.numpy as jnp
from jax import lax
from jax.experimental import pallas as pl
from jax.experimental.pallas import tpu as pltpu
from jax.sharding import PartitionSpec as P

MESH = pl.DeviceIdType.MESH
GROUP_AXES = ("model", "cols")

N_DEV = 128
N_COLS = 16
COL = 160
MID_COL = 144
OUT_COL = 40
BLOCKS = ((0, 4), (4, 4), (8, 4), (12, 2))
LAST = 14
C1 = 128
C2 = 256
HOPS = (0, 1, 2, 1)


def greet_order():
    shifts = [(dx, dy, dz) for dx in range(4) for dy in range(4) for dz in range(4)][1:]
    return sorted(shifts, key=lambda s: (-HOPS[s[1]] - HOPS[s[2]], -HOPS[s[0]]))


GREET_ORDER = greet_order()
LATER_Z = ((0, 3, 17, 11), (100, 100, 109, 105))
LATER_Y = ((20, 6, 0, 12), (17, 8, 0, 12))
LATER_X = ((-6, 0, -1, -2), (0.0, 0.31, 0.3, 0.1))
LATER_CORE = 0.5
MIX = (0, 1, 1, 1, 1, 1)
EARLY = (1, 2)


def send_order():
    def key(msg):
        window, dx, dy, z, dk = msg
        mix = (MIX[1] * window + MIX[2] * dx + MIX[3] * dy + MIX[4] * z) * (MIX[5] + dk) % 17
        return LATER_Z[window][z] + LATER_Y[window][dy] + LATER_X[window][dx] + LATER_CORE * dk + MIX[0] * mix

    windows = [(1, dx, dy, z, dk) for dx in range(4) for dy in range(4) for z in range(4) for dk in range(2)]
    weights = [(0, dx, dy, z, 0) for dx in range(4) for dy in range(4) for z in range(4)]
    order = sorted(weights + windows, key=key)
    return [m for m in order if m[3] == 0], [m for m in order if m[3] > 0]


SEND_ORDER = send_order()


def dot(a, b):
    return lax.dot_general(a, b, (((1,), (0,)), ((), ())), preferred_element_type=jnp.float32)


def kernel(x_hbm, w1_hbm, b1_hbm, w2_hbm, b2_hbm, out_ref, ys0, ys8, w2_mat,
           x_loc, w1_loc, b1_loc, b2_loc, turned, pick, sel, place, s_w, s_x, r_w, r_w2, r_x,
           w1_mat, tmp, edge, xs0, xs8, inside, res,
           heard, sem_x, sem_w1, sem_b, sem_w2, send_w, send_x, send_d, recv_w, recv_x, recv_d):
    m = lax.axis_index("model")
    c = lax.axis_index("cols")
    core = m % 2
    chip = m // 2 * N_COLS + c
    me = core * 64 + chip

    get_x = pltpu.make_async_copy(x_hbm, x_loc, sem_x)
    get_x.start()
    get_w1 = pltpu.make_async_copy(w1_hbm, w1_loc, sem_w1)
    get_w1.start()
    get_b = (pltpu.make_async_copy(b1_hbm, b1_loc, sem_b.at[0]), pltpu.make_async_copy(b2_hbm, b2_loc, sem_b.at[1]))
    for get in get_b:
        get.start()
    get_w2 = pltpu.make_async_copy(w2_hbm, w2_mat, sem_w2)
    get_w2.start()

    cores = (core, 1 - core)
    models = [[((m // 2 + dx) % 4) * 2 + k for k in cores] for dx in range(4)]
    ys = [(c % 4 + dy) % 4 for dy in range(4)]
    my_z = c // 4
    zs = [((my_z + dz) % 4) * 4 for dz in range(4)]

    barrier = pltpu.get_barrier_semaphore()
    part = (my_z + 3) // 4
    partner = {"model": m + 1 - 2 * core, "cols": c}
    for dx, dy, dz in GREET_ORDER:
        to = {"model": ((m // 2 + dx) % 4) * 2 + part, "cols": zs[dz] + ys[dy]}
        pl.semaphore_signal(barrier, inc=1, device_id=to, device_id_type=MESH)
    pl.semaphore_signal(barrier, inc=1, device_id=partner, device_id_type=MESH)

    def hear(which):
        @pl.when(core == which)
        def _():
            pl.semaphore_wait(barrier, (32, 96)[which] - 1 + 2 * ((core + part) % 2))
            pl.semaphore_signal(heard, inc=1, device_id=partner, device_id_type=MESH)

        @pl.when(core != which)
        def _():
            pl.semaphore_wait(heard, 1)

    for blk in range(4):
        lane = blk * 512 + lax.broadcasted_iota(jnp.int32, (1, 512), 1)
        img = lane % 8
        if blk < 2:
            row = (lane // 128) * 16 + (lane // 8) % 16
        else:
            h = (lane // 8) % 4
            row = (lane // 128 - 8) * 16 + h - 2 + jnp.where(h >= 2, 16, 0)
        at = jnp.where((row >= 0) & (row < 128), img * 128 + row, -1)
        for pair in range(4):
            rows = pair * 256 + lax.broadcasted_iota(jnp.int32, (256, 512), 0)
            pick[pair * 256 : pair * 256 + 256, blk * 512 : blk * 512 + 512] = jnp.where(rows == at, 1.0, 0.0).astype(jnp.bfloat16)
    r_id = lax.broadcasted_iota(jnp.int32, (256, 256), 0)
    k_id = lax.broadcasted_iota(jnp.int32, (256, 256), 1)
    first = (r_id // 16) * 8 - 2
    s_id = r_id % 16
    main = (s_id < 12) & (k_id == first + s_id) & (k_id < 128)
    from_col = first + 4 * (s_id - 12)
    border = (s_id >= 12) & (s_id < 15) & (k_id >= 128 + jnp.maximum(from_col, 0)) & (k_id < 132 + from_col)
    place[...] = jnp.where(main | border, 1.0, 0.0).astype(jnp.bfloat16)
    get_w1.wait()
    for tap in range(9):
        s_w[tap] = jnp.concatenate([w1_loc[tap // 3, tap % 3 : tap % 3 + 1, half * 128 : half * 128 + 128] for half in range(2)])

    get_x.wait()
    for n in range(8):
        turned[:, n * 128 : n * 128 + 128] = x_loc[n].T
    w_id = lax.broadcasted_iota(jnp.int32, (128, 256), 0)
    l_id = lax.broadcasted_iota(jnp.int32, (128, 256), 1) % 128
    keep = (l_id // 32) == ((w_id + 2) % 4)
    for blk in range(8):
        z = None
        for pair in range(4):
            term = dot(turned[:, pair * 256 : pair * 256 + 256], pick[pair * 256 : pair * 256 + 256, blk * 256 : blk * 256 + 256])
            z = term if z is None else z + term
        if blk >= 4:
            z = jnp.where(keep, z, 0.0)
        top = 0 if blk < 4 else 128
        sel[top : top + 128, (blk % 4) * 256 : (blk % 4) * 256 + 256] = z.astype(jnp.bfloat16)
    for blk in range(4):
        t = dot(place[...], sel[:, blk * 256 : blk * 256 + 256])
        for r in range(2):
            tiles = t[:, r * 128 : r * 128 + 128].reshape(16, 2, 8, 128).astype(jnp.bfloat16)
            s_x[(blk * 2 + r) * 16 : (blk * 2 + r) * 16 + 16] = tiles


    def send(src, dst, send_sem, recv_sem, pm, pc):
        pltpu.make_async_remote_copy(src_ref=src, dst_ref=dst, send_sem=send_sem, recv_sem=recv_sem,
                                     device_id={"model": pm, "cols": pc}, device_id_type=MESH).start()

    for which, order in enumerate(SEND_ORDER):
        hear(which)
        served = set()
        for window, dx, dy, z, dk in order:
            if window and z in EARLY and z not in served:
                served.add(z)
                for k in (1, 0):
                    def send_early(pm=k, pc=z * 4):
                        send(s_x.at[pm * N_COLS + pc], r_x.at[me], send_x, recv_x, pm, pc)
                    pl.when((m != k) | (c != z * 4))(send_early)
            pm, pc = models[dx][dk], z * 4 + ys[dy]

            def send_one(window=window, pm=pm, pc=pc):
                if window:
                    send(s_x.at[pm * N_COLS + pc], r_x.at[me], send_x, recv_x, pm, pc)
                else:
                    send(s_w, r_w.at[chip], send_w, recv_w, pm, pc)

            conds = []
            if dx == dy == dk == 0:
                conds.append(my_z != z)
            if window and z in EARLY:
                conds.append(models[dx][0] // 2 + ys[dy] != 0)
            if conds:
                pl.when(functools.reduce(lambda p, q: p & q, conds))(send_one)
            else:
                send_one()
    r_w[pl.ds(chip, 1)] = s_w[...].reshape(1, 9, 2, 128)
    r_x[pl.ds(me, 1)] = s_x[pl.ds(m * N_COLS + c, 1)]

    at_row = m * 16 - 1 + lax.broadcasted_iota(jnp.int32, (10, MID_COL, 128), 1) // 8
    at_col = c * 8 - 1 + lax.broadcasted_iota(jnp.int32, (10, MID_COL, 128), 0)
    inside[...] = jnp.where((at_row >= 0) & (at_row < 128) & (at_col >= 0) & (at_col < 128), 1.0, 0.0)

    def drain(ref, count, sem):
        part = ref.at[pl.ds(0, count)]
        pltpu.make_async_copy(part, part, sem).wait()

    def unpack_w(ref, k):
        for tap in range(9):
            tmp[0, 0:N_DEV] = ref[:, tap].astype(jnp.float32).reshape(N_DEV, 128)
            at = pl.multiple_of(tap * C1 + k * 64, 64)
            for half in range(2):
                w1_mat[pl.ds(at, 64), half * 128 : half * 128 + 128] = tmp.at[0][pl.ds(half, 64, stride=2), :].astype(jnp.bfloat16)

    drain(r_w, 63, recv_w)
    swap = pltpu.make_async_remote_copy(src_ref=r_w, dst_ref=r_w2, send_sem=send_d, recv_sem=recv_d,
                                        device_id=partner, device_id_type=MESH)
    swap.start()
    unpack_w(r_w, core)
    swap.wait_recv()
    unpack_w(r_w2, 1 - core)
    for get in get_b:
        get.wait()
    get_w2.wait()

    drain(r_x, N_DEV - 1, recv_x)
    for half in range(2):
        tmp[half] = r_x[:, half].astype(jnp.float32).reshape(N_DEV * 8, 128)

    def pixels(s):
        return tmp.at[s // 8][pl.ds(s % 8, N_DEV, stride=8), :].T

    for s in range(12, 15):
        edge[s - 12] = pixels(s)
    for w in range(12):
        top = (w % 4) * 32
        col = jnp.concatenate([edge[w // 4, top : top + 16], pixels(w), edge[w // 4, top + 16 : top + 32]])
        xs0[w] = col.astype(jnp.bfloat16)
        xs8[w] = col[8 : 8 + MID_COL].astype(jnp.bfloat16)

    before = None
    for top, rows in ((0, 48), (48, 32), (80, 32), (112, 32)):
        acc = None
        for pair in range(5):
            lhs = []
            for tap in range(2 * pair, min(2 * pair + 2, 9)):
                dh, dw = tap // 3, tap % 3
                src = xs8 if dh == 1 else xs0
                at = top + (16 if dh == 2 else 0)
                lhs.append(src[dw : dw + 10, at : at + rows].reshape(10 * rows, C1))
            lhs = jnp.concatenate(lhs, axis=1) if len(lhs) > 1 else lhs[0]
            term = dot(lhs, w1_mat[pair * 256 : pair * 256 + lhs.shape[1], :])
            acc = term if acc is None else acc + term
        act = jnp.maximum(acc + b1_loc[...], 0.0).reshape(10, rows, C2)
        ok = inside[:, top : top + rows] > 0.0
        real = [jnp.where(ok, act[:, :, half * 128 : half * 128 + 128], 0.0) for half in range(2)]
        for half in range(2):
            part = slice(half * 128, half * 128 + 128)
            ys0[:, top : top + rows, part] = real[half].astype(jnp.bfloat16)
            if before is None:
                ys8[:, 0 : rows - 16, part] = real[half][:, 8 : rows - 8].astype(jnp.bfloat16)
            else:
                shifted = jnp.concatenate([before[half], real[half][:, 0 : rows - 8]], axis=1)
                ys8[:, top - 16 : top + rows - 16, part] = shifted.astype(jnp.bfloat16)
        before = [r[:, rows - 8 :] for r in real]

    for i, (top, rows) in enumerate(BLOCKS):
        conv_two(top, rows, 1, ys0, ys8, w2_mat, b2_loc, res.at[i], out_ref)

    drain(r_w, 63, send_w)
    drain(s_x, N_DEV - 1, send_x)
    swap.wait_send()


def conv_two(top, rows, parts, ys0, ys8, w2_mat, b2_ref, res, out_ref):
    cols = 8 // parts
    size = rows * 8
    for part in range(parts):
        acc = None
        for tap in range(9):
            dh, dw = tap // 3, tap % 3
            src = ys8 if dh == 1 else ys0
            at = top * 8 + (16 if dh == 2 else 0)
            lo = dw + part * cols
            term = dot(src[lo : lo + cols, at : at + size].reshape(cols * size, C2), w2_mat[dh, dw])
            acc = term if acc is None else acc + term
        full = acc + b2_ref[...]
        for w in range(cols):
            for half in range(2):
                to = (part * cols + w) * (size + 8)
                res[half, to : to + size] = full[w * size : w * size + size, half * 128 : half * 128 + 128]
    for h in range(rows):
        for n in range(8):
            for half in range(2):
                vals = res.at[half][pl.ds(h * 8 + n, 8, stride=size + 8), :]
                out_ref[n, top % out_ref.shape[1] + h, :, half * 128 : half * 128 + 128] = vals


def kernel_two(out_a, ys0, ys8, w2_mat, b2_ref, out_hbm, out_b, res, sem):
    put_a = pltpu.make_async_copy(out_a, out_hbm.at[:, 0:LAST], sem.at[0])
    put_a.start()
    conv_two(LAST, 16 - LAST, 1, ys0, ys8, w2_mat, b2_ref, res, out_b)
    put_b = pltpu.make_async_copy(out_b, out_hbm.at[:, LAST:16], sem.at[1])
    put_b.start()
    put_a.wait()
    put_b.wait()


def solution(mesh):
    def run_local(x_in, w_conv1, b_conv1, w_conv2, b_conv2):
        bf, f32 = jnp.bfloat16, jnp.float32
        vmem = pl.BlockSpec(memory_space=pltpu.VMEM)
        hbm = pl.BlockSpec(memory_space=pltpu.HBM)
        dma = pltpu.SemaphoreType.DMA
        operands = (x_in.reshape(x_in.shape[:3]), w_conv1.reshape(3, 3, C2), b_conv1.reshape(1, C2), w_conv2, b_conv2.reshape(1, C2))
        out_a, ys0, ys8, w2 = pl.pallas_call(
            kernel,
            name="conv_pair",
            out_shape=[
                jax.ShapeDtypeStruct((8, LAST, 8, C2), f32),
                jax.ShapeDtypeStruct((10, MID_COL, C2), bf),
                jax.ShapeDtypeStruct((10, 128, C2), bf),
                jax.ShapeDtypeStruct((3, 3, C2, C2), bf),
            ],
            in_specs=[hbm] * 5,
            out_specs=[vmem] * 4,
            scratch_shapes=[
                pltpu.VMEM((8, 128, 128), bf),
                pltpu.VMEM((3, 3, C2), bf),
                pltpu.VMEM((1, C2), f32),
                pltpu.VMEM((1, C2), f32),
                pltpu.VMEM((128, 1024), bf),
                pltpu.VMEM((1024, 2048), bf),
                pltpu.VMEM((256, 1024), bf),
                pltpu.VMEM((256, 256), bf),
                pltpu.VMEM((9, 2, 128), bf),
                pltpu.VMEM((N_DEV, 2, 8, 128), bf),
                pltpu.VMEM((64, 9, 2, 128), bf),
                pltpu.VMEM((64, 9, 2, 128), bf),
                pltpu.VMEM((N_DEV, 2, 8, 128), bf),
                pltpu.VMEM((9 * C1, C2), bf),
                pltpu.VMEM((2, N_DEV * 8, 128), f32),
                pltpu.VMEM((3, 128, 128), f32),
                pltpu.VMEM((12, COL, C1), bf),
                pltpu.VMEM((12, MID_COL, C1), bf),
                pltpu.VMEM((10, MID_COL, 128), f32),
                pltpu.VMEM((len(BLOCKS), 2, 8 * OUT_COL, 128), f32),
                pltpu.SemaphoreType.REGULAR, dma, dma, pltpu.SemaphoreType.DMA((2,)), dma,
                dma, dma, dma, dma, dma, dma,
            ],
            compiler_params=pltpu.CompilerParams(collective_id=0, has_side_effects=True, vmem_limit_bytes=24 << 20),
        )(*(pltpu.with_memory_space_constraint(a, pltpu.HBM) for a in operands))
        return pl.pallas_call(
            kernel_two,
            name="conv_last",
            out_shape=jax.ShapeDtypeStruct((8, 16, 8, C2), f32),
            in_specs=[vmem] * 5,
            out_specs=hbm,
            scratch_shapes=[pltpu.VMEM((8, 16 - LAST, 8, C2), f32), pltpu.VMEM((2, 8 * OUT_COL, 128), f32), pltpu.SemaphoreType.DMA((2,))],
            compiler_params=pltpu.CompilerParams(vmem_limit_bytes=24 << 20),
        )(out_a, ys0, ys8, w2, operands[-1])

    return jax.shard_map(
        run_local,
        mesh=mesh,
        in_specs=(P("data", None, None, GROUP_AXES), P(None, None, GROUP_AXES, None), P(), P(), P()),
        out_specs=P("data", "model", "cols", None),
        check_vma=False,
    )
```

```python
import collections
import functools

import jax
import jax.numpy as jnp
from jax import lax
from jax.experimental import pallas as pl
from jax.experimental.pallas import tpu as pltpu
from jax.sharding import PartitionSpec as P

MESH = pl.DeviceIdType.MESH
GROUP_AXES = ("model", "cols")

N_DEV = 128
N_COLS = 16
COL = 160
MID_COL = 144
OUT_COL = 40
BLOCKS = ((0, 4), (4, 4), (8, 4), (12, 2))
LAST = 14
C1 = 128
C2 = 256
HOPS = (0, 1, 2, 1)


def greet_order():
    shifts = [(dx, dy, dz) for dx in range(4) for dy in range(4) for dz in range(4)][1:]
    return sorted(shifts, key=lambda s: (-HOPS[s[1]] - HOPS[s[2]], -HOPS[s[0]]))


GREET_ORDER = greet_order()
LATER_Z = ((0, 3, 17, 11), (100, 100, 109, 105))
LATER_Y = ((20, 6, 0, 12), (17, 8, 0, 12))
LATER_X = ((-6, 0, -1, -2), (0.0, 0.31, 0.3, 0.1))
LATER_CORE = 0.5
MIX = (0, 1, 1, 1, 1, 1)
EARLY = (1, 2, 3)


def send_order():
    def key(msg):
        window, dx, dy, z, dk = msg
        mix = (MIX[1] * window + MIX[2] * dx + MIX[3] * dy + MIX[4] * z) * (MIX[5] + dk) % 17
        return LATER_Z[window][z] + LATER_Y[window][dy] + LATER_X[window][dx] + LATER_CORE * dk + MIX[0] * mix

    windows = [(1, dx, dy, z, dk) for dx in range(4) for dy in range(4) for z in range(4) for dk in range(2)]
    weights = [(0, dx, dy, z, 0) for dx in range(4) for dy in range(4) for z in range(4)]
    order = sorted(weights + windows, key=key)
    return [m for m in order if m[3] == 0], [m for m in order if m[3] > 0]


SEND_ORDER = send_order()


def dot(a, b):
    return lax.dot_general(a, b, (((1,), (0,)), ((), ())), preferred_element_type=jnp.float32)


def kernel(x_hbm, w1_hbm, b1_hbm, w2_hbm, b2_hbm, out_ref, ys0, ys8, w2_mat,
           x_loc, w1_loc, b1_loc, b2_loc, turned, pick, sel, place, s_w, s_x, r_w, r_w2, r_x,
           w1_mat, tmp, edge, xs0, xs8, inside, res,
           heard, sem_x, sem_w1, sem_b, sem_w2, send_w, send_x, send_d, recv_w, recv_x, recv_d):
    m = lax.axis_index("model")
    c = lax.axis_index("cols")
    core = m % 2
    chip = m // 2 * N_COLS + c
    me = core * 64 + chip

    get_x = pltpu.make_async_copy(x_hbm, x_loc, sem_x)
    get_x.start()
    get_w1 = pltpu.make_async_copy(w1_hbm, w1_loc, sem_w1)
    get_w1.start()
    get_b = (pltpu.make_async_copy(b1_hbm, b1_loc, sem_b.at[0]), pltpu.make_async_copy(b2_hbm, b2_loc, sem_b.at[1]))
    for get in get_b:
        get.start()
    get_w2 = pltpu.make_async_copy(w2_hbm, w2_mat, sem_w2)
    get_w2.start()

    cores = (core, 1 - core)
    models = [[((m // 2 + dx) % 4) * 2 + k for k in cores] for dx in range(4)]
    ys = [(c % 4 + dy) % 4 for dy in range(4)]
    my_z = c // 4
    zs = [((my_z + dz) % 4) * 4 for dz in range(4)]

    barrier = pltpu.get_barrier_semaphore()
    part = (my_z + 3) // 4
    partner = {"model": m + 1 - 2 * core, "cols": c}
    for dx, dy, dz in GREET_ORDER:
        to = {"model": ((m // 2 + dx) % 4) * 2 + part, "cols": zs[dz] + ys[dy]}
        pl.semaphore_signal(barrier, inc=1, device_id=to, device_id_type=MESH)
    pl.semaphore_signal(barrier, inc=1, device_id=partner, device_id_type=MESH)

    def hear(which):
        @pl.when(core == which)
        def _():
            pl.semaphore_wait(barrier, (32, 96)[which] - 1 + 2 * ((core + part) % 2))
            pl.semaphore_signal(heard, inc=1, device_id=partner, device_id_type=MESH)

        @pl.when(core != which)
        def _():
            pl.semaphore_wait(heard, 1)

    for blk in range(4):
        lane = blk * 512 + lax.broadcasted_iota(jnp.int32, (1, 512), 1)
        img = lane % 8
        if blk < 2:
            row = (lane // 128) * 16 + (lane // 8) % 16
        else:
            h = (lane // 8) % 4
            row = (lane // 128 - 8) * 16 + h - 2 + jnp.where(h >= 2, 16, 0)
        at = jnp.where((row >= 0) & (row < 128), img * 128 + row, -1)
        for pair in range(4):
            rows = pair * 256 + lax.broadcasted_iota(jnp.int32, (256, 512), 0)
            pick[pair * 256 : pair * 256 + 256, blk * 512 : blk * 512 + 512] = jnp.where(rows == at, 1.0, 0.0).astype(jnp.bfloat16)
    r_id = lax.broadcasted_iota(jnp.int32, (256, 256), 0)
    k_id = lax.broadcasted_iota(jnp.int32, (256, 256), 1)
    first = (r_id // 16) * 8 - 2
    s_id = r_id % 16
    main = (s_id < 12) & (k_id == first + s_id) & (k_id < 128)
    from_col = first + 4 * (s_id - 12)
    border = (s_id >= 12) & (s_id < 15) & (k_id >= 128 + jnp.maximum(from_col, 0)) & (k_id < 132 + from_col)
    place[...] = jnp.where(main | border, 1.0, 0.0).astype(jnp.bfloat16)
    get_w1.wait()
    for tap in range(9):
        s_w[tap] = jnp.concatenate([w1_loc[tap // 3, tap % 3 : tap % 3 + 1, half * 128 : half * 128 + 128] for half in range(2)])

    get_x.wait()
    for n in range(8):
        turned[:, n * 128 : n * 128 + 128] = x_loc[n].T
    w_id = lax.broadcasted_iota(jnp.int32, (128, 256), 0)
    l_id = lax.broadcasted_iota(jnp.int32, (128, 256), 1) % 128
    keep = (l_id // 32) == ((w_id + 2) % 4)
    for blk in range(8):
        z = None
        for pair in range(4):
            term = dot(turned[:, pair * 256 : pair * 256 + 256], pick[pair * 256 : pair * 256 + 256, blk * 256 : blk * 256 + 256])
            z = term if z is None else z + term
        if blk >= 4:
            z = jnp.where(keep, z, 0.0)
        top = 0 if blk < 4 else 128
        sel[top : top + 128, (blk % 4) * 256 : (blk % 4) * 256 + 256] = z.astype(jnp.bfloat16)
    for blk in range(4):
        t = dot(place[...], sel[:, blk * 256 : blk * 256 + 256])
        for r in range(2):
            tiles = t[:, r * 128 : r * 128 + 128].reshape(16, 2, 8, 128).astype(jnp.bfloat16)
            s_x[(blk * 2 + r) * 16 : (blk * 2 + r) * 16 + 16] = tiles


    def send(src, dst, send_sem, recv_sem, pm, pc):
        pltpu.make_async_remote_copy(src_ref=src, dst_ref=dst, send_sem=send_sem, recv_sem=recv_sem,
                                     device_id={"model": pm, "cols": pc}, device_id_type=MESH).start()

    for which, order in enumerate(SEND_ORDER):
        hear(which)
        served = set()
        for window, dx, dy, z, dk in order:
            if window and z in EARLY and z not in served:
                served.add(z)
                for k in (1, 0):
                    def send_early(pm=k, pc=z * 4):
                        send(s_x.at[pm * N_COLS + pc], r_x.at[me], send_x, recv_x, pm, pc)
                    pl.when((m != k) | (c != z * 4))(send_early)
            pm, pc = models[dx][dk], z * 4 + ys[dy]

            def send_one(window=window, pm=pm, pc=pc):
                if window:
                    send(s_x.at[pm * N_COLS + pc], r_x.at[me], send_x, recv_x, pm, pc)
                else:
                    send(s_w, r_w.at[chip], send_w, recv_w, pm, pc)

            conds = []
            if dx == dy == dk == 0:
                conds.append(my_z != z)
            if window and z in EARLY:
                conds.append(models[dx][0] // 2 + ys[dy] != 0)
            if conds:
                pl.when(functools.reduce(lambda p, q: p & q, conds))(send_one)
            else:
                send_one()
    r_w[pl.ds(chip, 1)] = s_w[...].reshape(1, 9, 2, 128)
    r_x[pl.ds(me, 1)] = s_x[pl.ds(m * N_COLS + c, 1)]

    at_row = m * 16 - 1 + lax.broadcasted_iota(jnp.int32, (10, MID_COL, 128), 1) // 8
    at_col = c * 8 - 1 + lax.broadcasted_iota(jnp.int32, (10, MID_COL, 128), 0)
    inside[...] = jnp.where((at_row >= 0) & (at_row < 128) & (at_col >= 0) & (at_col < 128), 1.0, 0.0)

    def drain(ref, count, sem):
        part = ref.at[pl.ds(0, count)]
        pltpu.make_async_copy(part, part, sem).wait()

    def unpack_w(ref, k):
        for tap in range(9):
            tmp[0, 0:N_DEV] = ref[:, tap].astype(jnp.float32).reshape(N_DEV, 128)
            at = pl.multiple_of(tap * C1 + k * 64, 64)
            for half in range(2):
                w1_mat[pl.ds(at, 64), half * 128 : half * 128 + 128] = tmp.at[0][pl.ds(half, 64, stride=2), :].astype(jnp.bfloat16)

    drain(r_w, 63, recv_w)
    swap = pltpu.make_async_remote_copy(src_ref=r_w, dst_ref=r_w2, send_sem=send_d, recv_sem=recv_d,
                                        device_id=partner, device_id_type=MESH)
    swap.start()
    unpack_w(r_w, core)
    swap.wait_recv()
    unpack_w(r_w2, 1 - core)
    for get in get_b:
        get.wait()
    get_w2.wait()

    drain(r_x, N_DEV - 1, recv_x)
    for half in range(2):
        tmp[half] = r_x[:, half].astype(jnp.float32).reshape(N_DEV * 8, 128)

    def pixels(s):
        return tmp.at[s // 8][pl.ds(s % 8, N_DEV, stride=8), :].T

    for s in range(12, 15):
        edge[s - 12] = pixels(s)
    for w in range(12):
        top = (w % 4) * 32
        col = jnp.concatenate([edge[w // 4, top : top + 16], pixels(w), edge[w // 4, top + 16 : top + 32]])
        xs0[w] = col.astype(jnp.bfloat16)
        xs8[w] = col[8 : 8 + MID_COL].astype(jnp.bfloat16)

    before = None
    for top, rows in ((0, 48), (48, 32), (80, 32), (112, 32)):
        acc = None
        for pair in range(5):
            lhs = []
            for tap in range(2 * pair, min(2 * pair + 2, 9)):
                dh, dw = tap // 3, tap % 3
                src = xs8 if dh == 1 else xs0
                at = top + (16 if dh == 2 else 0)
                lhs.append(src[dw : dw + 10, at : at + rows].reshape(10 * rows, C1))
            lhs = jnp.concatenate(lhs, axis=1) if len(lhs) > 1 else lhs[0]
            term = dot(lhs, w1_mat[pair * 256 : pair * 256 + lhs.shape[1], :])
            acc = term if acc is None else acc + term
        act = jnp.maximum(acc + b1_loc[...], 0.0).reshape(10, rows, C2)
        ok = inside[:, top : top + rows] > 0.0
        real = [jnp.where(ok, act[:, :, half * 128 : half * 128 + 128], 0.0) for half in range(2)]
        for half in range(2):
            part = slice(half * 128, half * 128 + 128)
            ys0[:, top : top + rows, part] = real[half].astype(jnp.bfloat16)
            if before is None:
                ys8[:, 0 : rows - 16, part] = real[half][:, 8 : rows - 8].astype(jnp.bfloat16)
            else:
                shifted = jnp.concatenate([before[half], real[half][:, 0 : rows - 8]], axis=1)
                ys8[:, top - 16 : top + rows - 16, part] = shifted.astype(jnp.bfloat16)
        before = [r[:, rows - 8 :] for r in real]

    for i, (top, rows) in enumerate(BLOCKS):
        conv_two(top, rows, 1, ys0, ys8, w2_mat, b2_loc, res.at[i], out_ref)

    drain(r_w, 63, send_w)
    drain(s_x, N_DEV - 1, send_x)
    swap.wait_send()


def conv_two(top, rows, parts, ys0, ys8, w2_mat, b2_ref, res, out_ref):
    cols = 8 // parts
    size = rows * 8
    for part in range(parts):
        acc = None
        for tap in range(9):
            dh, dw = tap // 3, tap % 3
            src = ys8 if dh == 1 else ys0
            at = top * 8 + (16 if dh == 2 else 0)
            lo = dw + part * cols
            term = dot(src[lo : lo + cols, at : at + size].reshape(cols * size, C2), w2_mat[dh, dw])
            acc = term if acc is None else acc + term
        full = acc + b2_ref[...]
        for w in range(cols):
            for half in range(2):
                to = (part * cols + w) * (size + 8)
                res[half, to : to + size] = full[w * size : w * size + size, half * 128 : half * 128 + 128]
    for h in range(rows):
        for n in range(8):
            for half in range(2):
                vals = res.at[half][pl.ds(h * 8 + n, 8, stride=size + 8), :]
                out_ref[n, top % out_ref.shape[1] + h, :, half * 128 : half * 128 + 128] = vals


def kernel_two(out_a, ys0, ys8, w2_mat, b2_ref, out_hbm, out_b, res, sem):
    put_a = pltpu.make_async_copy(out_a, out_hbm.at[:, 0:LAST], sem.at[0])
    put_a.start()
    conv_two(LAST, 16 - LAST, 1, ys0, ys8, w2_mat, b2_ref, res, out_b)
    put_b = pltpu.make_async_copy(out_b, out_hbm.at[:, LAST:16], sem.at[1])
    put_b.start()
    put_a.wait()
    put_b.wait()


def solution(mesh):
    def run_local(x_in, w_conv1, b_conv1, w_conv2, b_conv2):
        bf, f32 = jnp.bfloat16, jnp.float32
        vmem = pl.BlockSpec(memory_space=pltpu.VMEM)
        hbm = pl.BlockSpec(memory_space=pltpu.HBM)
        dma = pltpu.SemaphoreType.DMA
        operands = (x_in.reshape(x_in.shape[:3]), w_conv1.reshape(3, 3, C2), b_conv1.reshape(1, C2), w_conv2, b_conv2.reshape(1, C2))
        out_a, ys0, ys8, w2 = pl.pallas_call(
            kernel,
            name="conv_pair",
            out_shape=[
                jax.ShapeDtypeStruct((8, LAST, 8, C2), f32),
                jax.ShapeDtypeStruct((10, MID_COL, C2), bf),
                jax.ShapeDtypeStruct((10, 128, C2), bf),
                jax.ShapeDtypeStruct((3, 3, C2, C2), bf),
            ],
            in_specs=[hbm] * 5,
            out_specs=[vmem] * 4,
            scratch_shapes=[
                pltpu.VMEM((8, 128, 128), bf),
                pltpu.VMEM((3, 3, C2), bf),
                pltpu.VMEM((1, C2), f32),
                pltpu.VMEM((1, C2), f32),
                pltpu.VMEM((128, 1024), bf),
                pltpu.VMEM((1024, 2048), bf),
                pltpu.VMEM((256, 1024), bf),
                pltpu.VMEM((256, 256), bf),
                pltpu.VMEM((9, 2, 128), bf),
                pltpu.VMEM((N_DEV, 2, 8, 128), bf),
                pltpu.VMEM((64, 9, 2, 128), bf),
                pltpu.VMEM((64, 9, 2, 128), bf),
                pltpu.VMEM((N_DEV, 2, 8, 128), bf),
                pltpu.VMEM((9 * C1, C2), bf),
                pltpu.VMEM((2, N_DEV * 8, 128), f32),
                pltpu.VMEM((3, 128, 128), f32),
                pltpu.VMEM((12, COL, C1), bf),
                pltpu.VMEM((12, MID_COL, C1), bf),
                pltpu.VMEM((10, MID_COL, 128), f32),
                pltpu.VMEM((len(BLOCKS), 2, 8 * OUT_COL, 128), f32),
                pltpu.SemaphoreType.REGULAR, dma, dma, pltpu.SemaphoreType.DMA((2,)), dma,
                dma, dma, dma, dma, dma, dma,
            ],
            compiler_params=pltpu.CompilerParams(collective_id=0, has_side_effects=True, vmem_limit_bytes=24 << 20),
        )(*(pltpu.with_memory_space_constraint(a, pltpu.HBM) for a in operands))
        return pl.pallas_call(
            kernel_two,
            name="conv_last",
            out_shape=jax.ShapeDtypeStruct((8, 16, 8, C2), f32),
            in_specs=[vmem] * 5,
            out_specs=hbm,
            scratch_shapes=[pltpu.VMEM((8, 16 - LAST, 8, C2), f32), pltpu.VMEM((2, 8 * OUT_COL, 128), f32), pltpu.SemaphoreType.DMA((2,))],
            compiler_params=pltpu.CompilerParams(vmem_limit_bytes=24 << 20),
        )(out_a, ys0, ys8, w2, operands[-1])

    return jax.shard_map(
        run_local,
        mesh=mesh,
        in_specs=(P("data", None, None, GROUP_AXES), P(None, None, GROUP_AXES, None), P(), P(), P()),
        out_specs=P("data", "model", "cols", None),
        check_vma=False,
    )
```

```python
import collections
import functools

import jax
import jax.numpy as jnp
from jax import lax
from jax.experimental import pallas as pl
from jax.experimental.pallas import tpu as pltpu
from jax.sharding import PartitionSpec as P

MESH = pl.DeviceIdType.MESH
GROUP_AXES = ("model", "cols")

N_DEV = 128
N_COLS = 16
COL = 160
MID_COL = 144
OUT_COL = 40
BLOCKS = ((0, 4), (4, 4), (8, 4), (12, 2))
LAST = 14
C1 = 128
C2 = 256
HOPS = (0, 1, 2, 1)


def greet_order():
    shifts = [(dx, dy, dz) for dx in range(4) for dy in range(4) for dz in range(4)][1:]
    return sorted(shifts, key=lambda s: (-HOPS[s[1]] - HOPS[s[2]], -HOPS[s[0]]))


GREET_ORDER = greet_order()
LATER_Z = ((0, 3, 17, 11), (100, 100, 109, 104))
LATER_Y = ((20, 6, 0, 12), (17, 8, 0, 12))
LATER_X = ((-6, 0, -1, -2), (0.0, 0.31, 0.3, 0.1))
LATER_CORE = 0.5
MIX = (0, 1, 1, 1, 1, 1)
EARLY = (1, 2)


def send_order():
    def key(msg):
        window, dx, dy, z, dk = msg
        mix = (MIX[1] * window + MIX[2] * dx + MIX[3] * dy + MIX[4] * z) * (MIX[5] + dk) % 17
        return LATER_Z[window][z] + LATER_Y[window][dy] + LATER_X[window][dx] + LATER_CORE * dk + MIX[0] * mix

    windows = [(1, dx, dy, z, dk) for dx in range(4) for dy in range(4) for z in range(4) for dk in range(2)]
    weights = [(0, dx, dy, z, 0) for dx in range(4) for dy in range(4) for z in range(4)]
    order = sorted(weights + windows, key=key)
    return [m for m in order if m[3] == 0], [m for m in order if m[3] > 0]


SEND_ORDER = send_order()


def dot(a, b):
    return lax.dot_general(a, b, (((1,), (0,)), ((), ())), preferred_element_type=jnp.float32)


def kernel(x_hbm, w1_hbm, b1_hbm, w2_hbm, b2_hbm, out_ref, ys0, ys8, w2_mat,
           x_loc, w1_loc, b1_loc, b2_loc, turned, pick, sel, place, s_w, s_x, r_w, r_w2, r_x,
           w1_mat, tmp, edge, xs0, xs8, inside, res,
           heard, sem_x, sem_w1, sem_b, sem_w2, send_w, send_x, send_d, recv_w, recv_x, recv_d):
    m = lax.axis_index("model")
    c = lax.axis_index("cols")
    core = m % 2
    chip = m // 2 * N_COLS + c
    me = core * 64 + chip

    get_x = pltpu.make_async_copy(x_hbm, x_loc, sem_x)
    get_x.start()
    get_w1 = pltpu.make_async_copy(w1_hbm, w1_loc, sem_w1)
    get_w1.start()
    get_b = (pltpu.make_async_copy(b1_hbm, b1_loc, sem_b.at[0]), pltpu.make_async_copy(b2_hbm, b2_loc, sem_b.at[1]))
    for get in get_b:
        get.start()
    get_w2 = pltpu.make_async_copy(w2_hbm, w2_mat, sem_w2)
    get_w2.start()

    cores = (core, 1 - core)
    models = [[((m // 2 + dx) % 4) * 2 + k for k in cores] for dx in range(4)]
    ys = [(c % 4 + dy) % 4 for dy in range(4)]
    my_z = c // 4
    zs = [((my_z + dz) % 4) * 4 for dz in range(4)]

    barrier = pltpu.get_barrier_semaphore()
    part = (my_z + 3) // 4
    partner = {"model": m + 1 - 2 * core, "cols": c}
    for dx, dy, dz in GREET_ORDER:
        to = {"model": ((m // 2 + dx) % 4) * 2 + part, "cols": zs[dz] + ys[dy]}
        pl.semaphore_signal(barrier, inc=1, device_id=to, device_id_type=MESH)
    pl.semaphore_signal(barrier, inc=1, device_id=partner, device_id_type=MESH)

    def hear(which):
        @pl.when(core == which)
        def _():
            pl.semaphore_wait(barrier, (32, 96)[which] - 1 + 2 * ((core + part) % 2))
            pl.semaphore_signal(heard, inc=1, device_id=partner, device_id_type=MESH)

        @pl.when(core != which)
        def _():
            pl.semaphore_wait(heard, 1)

    for blk in range(4):
        lane = blk * 512 + lax.broadcasted_iota(jnp.int32, (1, 512), 1)
        img = lane % 8
        if blk < 2:
            row = (lane // 128) * 16 + (lane // 8) % 16
        else:
            h = (lane // 8) % 4
            row = (lane // 128 - 8) * 16 + h - 2 + jnp.where(h >= 2, 16, 0)
        at = jnp.where((row >= 0) & (row < 128), img * 128 + row, -1)
        for pair in range(4):
            rows = pair * 256 + lax.broadcasted_iota(jnp.int32, (256, 512), 0)
            pick[pair * 256 : pair * 256 + 256, blk * 512 : blk * 512 + 512] = jnp.where(rows == at, 1.0, 0.0).astype(jnp.bfloat16)
    r_id = lax.broadcasted_iota(jnp.int32, (256, 256), 0)
    k_id = lax.broadcasted_iota(jnp.int32, (256, 256), 1)
    first = (r_id // 16) * 8 - 2
    s_id = r_id % 16
    main = (s_id < 12) & (k_id == first + s_id) & (k_id < 128)
    from_col = first + 4 * (s_id - 12)
    border = (s_id >= 12) & (s_id < 15) & (k_id >= 128 + jnp.maximum(from_col, 0)) & (k_id < 132 + from_col)
    place[...] = jnp.where(main | border, 1.0, 0.0).astype(jnp.bfloat16)
    get_w1.wait()
    for tap in range(9):
        s_w[tap] = jnp.concatenate([w1_loc[tap // 3, tap % 3 : tap % 3 + 1, half * 128 : half * 128 + 128] for half in range(2)])

    get_x.wait()
    for n in range(8):
        turned[:, n * 128 : n * 128 + 128] = x_loc[n].T
    w_id = lax.broadcasted_iota(jnp.int32, (128, 256), 0)
    l_id = lax.broadcasted_iota(jnp.int32, (128, 256), 1) % 128
    keep = (l_id // 32) == ((w_id + 2) % 4)
    for blk in range(8):
        z = None
        for pair in range(4):
            term = dot(turned[:, pair * 256 : pair * 256 + 256], pick[pair * 256 : pair * 256 + 256, blk * 256 : blk * 256 + 256])
            z = term if z is None else z + term
        if blk >= 4:
            z = jnp.where(keep, z, 0.0)
        top = 0 if blk < 4 else 128
        sel[top : top + 128, (blk % 4) * 256 : (blk % 4) * 256 + 256] = z.astype(jnp.bfloat16)
    for blk in range(4):
        t = dot(place[...], sel[:, blk * 256 : blk * 256 + 256])
        for r in range(2):
            tiles = t[:, r * 128 : r * 128 + 128].reshape(16, 2, 8, 128).astype(jnp.bfloat16)
            s_x[(blk * 2 + r) * 16 : (blk * 2 + r) * 16 + 16] = tiles


    def send(src, dst, send_sem, recv_sem, pm, pc):
        pltpu.make_async_remote_copy(src_ref=src, dst_ref=dst, send_sem=send_sem, recv_sem=recv_sem,
                                     device_id={"model": pm, "cols": pc}, device_id_type=MESH).start()

    for which, order in enumerate(SEND_ORDER):
        hear(which)
        served = set()
        for window, dx, dy, z, dk in order:
            if window and z in EARLY and z not in served:
                served.add(z)
                for k in (1, 0):
                    def send_early(pm=k, pc=z * 4):
                        send(s_x.at[pm * N_COLS + pc], r_x.at[me], send_x, recv_x, pm, pc)
                    pl.when((m != k) | (c != z * 4))(send_early)
            pm, pc = models[dx][dk], z * 4 + ys[dy]

            def send_one(window=window, pm=pm, pc=pc):
                if window:
                    send(s_x.at[pm * N_COLS + pc], r_x.at[me], send_x, recv_x, pm, pc)
                else:
                    send(s_w, r_w.at[chip], send_w, recv_w, pm, pc)

            conds = []
            if dx == dy == dk == 0:
                conds.append(my_z != z)
            if window and z in EARLY:
                conds.append(models[dx][0] // 2 + ys[dy] != 0)
            if conds:
                pl.when(functools.reduce(lambda p, q: p & q, conds))(send_one)
            else:
                send_one()
    r_w[pl.ds(chip, 1)] = s_w[...].reshape(1, 9, 2, 128)
    r_x[pl.ds(me, 1)] = s_x[pl.ds(m * N_COLS + c, 1)]

    at_row = m * 16 - 1 + lax.broadcasted_iota(jnp.int32, (10, MID_COL, 128), 1) // 8
    at_col = c * 8 - 1 + lax.broadcasted_iota(jnp.int32, (10, MID_COL, 128), 0)
    inside[...] = jnp.where((at_row >= 0) & (at_row < 128) & (at_col >= 0) & (at_col < 128), 1.0, 0.0)

    def drain(ref, count, sem):
        part = ref.at[pl.ds(0, count)]
        pltpu.make_async_copy(part, part, sem).wait()

    def unpack_w(ref, k):
        for tap in range(9):
            tmp[0, 0:N_DEV] = ref[:, tap].astype(jnp.float32).reshape(N_DEV, 128)
            at = pl.multiple_of(tap * C1 + k * 64, 64)
            for half in range(2):
                w1_mat[pl.ds(at, 64), half * 128 : half * 128 + 128] = tmp.at[0][pl.ds(half, 64, stride=2), :].astype(jnp.bfloat16)

    drain(r_w, 63, recv_w)
    swap = pltpu.make_async_remote_copy(src_ref=r_w, dst_ref=r_w2, send_sem=send_d, recv_sem=recv_d,
                                        device_id=partner, device_id_type=MESH)
    swap.start()
    unpack_w(r_w, core)
    swap.wait_recv()
    unpack_w(r_w2, 1 - core)
    for get in get_b:
        get.wait()
    get_w2.wait()

    drain(r_x, N_DEV - 1, recv_x)
    for half in range(2):
        tmp[half] = r_x[:, half].astype(jnp.float32).reshape(N_DEV * 8, 128)

    def pixels(s):
        return tmp.at[s // 8][pl.ds(s % 8, N_DEV, stride=8), :].T

    for s in range(12, 15):
        edge[s - 12] = pixels(s)
    for w in range(12):
        top = (w % 4) * 32
        col = jnp.concatenate([edge[w // 4, top : top + 16], pixels(w), edge[w // 4, top + 16 : top + 32]])
        xs0[w] = col.astype(jnp.bfloat16)
        xs8[w] = col[8 : 8 + MID_COL].astype(jnp.bfloat16)

    before = None
    for top, rows in ((0, 48), (48, 32), (80, 32), (112, 32)):
        acc = None
        for pair in range(5):
            lhs = []
            for tap in range(2 * pair, min(2 * pair + 2, 9)):
                dh, dw = tap // 3, tap % 3
                src = xs8 if dh == 1 else xs0
                at = top + (16 if dh == 2 else 0)
                lhs.append(src[dw : dw + 10, at : at + rows].reshape(10 * rows, C1))
            lhs = jnp.concatenate(lhs, axis=1) if len(lhs) > 1 else lhs[0]
            term = dot(lhs, w1_mat[pair * 256 : pair * 256 + lhs.shape[1], :])
            acc = term if acc is None else acc + term
        act = jnp.maximum(acc + b1_loc[...], 0.0).reshape(10, rows, C2)
        ok = inside[:, top : top + rows] > 0.0
        real = [jnp.where(ok, act[:, :, half * 128 : half * 128 + 128], 0.0) for half in range(2)]
        for half in range(2):
            part = slice(half * 128, half * 128 + 128)
            ys0[:, top : top + rows, part] = real[half].astype(jnp.bfloat16)
            if before is None:
                ys8[:, 0 : rows - 16, part] = real[half][:, 8 : rows - 8].astype(jnp.bfloat16)
            else:
                shifted = jnp.concatenate([before[half], real[half][:, 0 : rows - 8]], axis=1)
                ys8[:, top - 16 : top + rows - 16, part] = shifted.astype(jnp.bfloat16)
        before = [r[:, rows - 8 :] for r in real]

    for i, (top, rows) in enumerate(BLOCKS):
        conv_two(top, rows, 1, ys0, ys8, w2_mat, b2_loc, res.at[i], out_ref)

    drain(r_w, 63, send_w)
    drain(s_x, N_DEV - 1, send_x)
    swap.wait_send()


def conv_two(top, rows, parts, ys0, ys8, w2_mat, b2_ref, res, out_ref):
    cols = 8 // parts
    size = rows * 8
    for part in range(parts):
        acc = None
        for tap in range(9):
            dh, dw = tap // 3, tap % 3
            src = ys8 if dh == 1 else ys0
            at = top * 8 + (16 if dh == 2 else 0)
            lo = dw + part * cols
            term = dot(src[lo : lo + cols, at : at + size].reshape(cols * size, C2), w2_mat[dh, dw])
            acc = term if acc is None else acc + term
        full = acc + b2_ref[...]
        for w in range(cols):
            for half in range(2):
                to = (part * cols + w) * (size + 8)
                res[half, to : to + size] = full[w * size : w * size + size, half * 128 : half * 128 + 128]
    for h in range(rows):
        for n in range(8):
            for half in range(2):
                vals = res.at[half][pl.ds(h * 8 + n, 8, stride=size + 8), :]
                out_ref[n, top % out_ref.shape[1] + h, :, half * 128 : half * 128 + 128] = vals


def kernel_two(out_a, ys0, ys8, w2_mat, b2_ref, out_hbm, out_b, res, sem):
    put_a = pltpu.make_async_copy(out_a, out_hbm.at[:, 0:LAST], sem.at[0])
    put_a.start()
    conv_two(LAST, 16 - LAST, 1, ys0, ys8, w2_mat, b2_ref, res, out_b)
    put_b = pltpu.make_async_copy(out_b, out_hbm.at[:, LAST:16], sem.at[1])
    put_b.start()
    put_a.wait()
    put_b.wait()


def solution(mesh):
    def run_local(x_in, w_conv1, b_conv1, w_conv2, b_conv2):
        bf, f32 = jnp.bfloat16, jnp.float32
        vmem = pl.BlockSpec(memory_space=pltpu.VMEM)
        hbm = pl.BlockSpec(memory_space=pltpu.HBM)
        dma = pltpu.SemaphoreType.DMA
        operands = (x_in.reshape(x_in.shape[:3]), w_conv1.reshape(3, 3, C2), b_conv1.reshape(1, C2), w_conv2, b_conv2.reshape(1, C2))
        out_a, ys0, ys8, w2 = pl.pallas_call(
            kernel,
            name="conv_pair",
            out_shape=[
                jax.ShapeDtypeStruct((8, LAST, 8, C2), f32),
                jax.ShapeDtypeStruct((10, MID_COL, C2), bf),
                jax.ShapeDtypeStruct((10, 128, C2), bf),
                jax.ShapeDtypeStruct((3, 3, C2, C2), bf),
            ],
            in_specs=[hbm] * 5,
            out_specs=[vmem] * 4,
            scratch_shapes=[
                pltpu.VMEM((8, 128, 128), bf),
                pltpu.VMEM((3, 3, C2), bf),
                pltpu.VMEM((1, C2), f32),
                pltpu.VMEM((1, C2), f32),
                pltpu.VMEM((128, 1024), bf),
                pltpu.VMEM((1024, 2048), bf),
                pltpu.VMEM((256, 1024), bf),
                pltpu.VMEM((256, 256), bf),
                pltpu.VMEM((9, 2, 128), bf),
                pltpu.VMEM((N_DEV, 2, 8, 128), bf),
                pltpu.VMEM((64, 9, 2, 128), bf),
                pltpu.VMEM((64, 9, 2, 128), bf),
                pltpu.VMEM((N_DEV, 2, 8, 128), bf),
                pltpu.VMEM((9 * C1, C2), bf),
                pltpu.VMEM((2, N_DEV * 8, 128), f32),
                pltpu.VMEM((3, 128, 128), f32),
                pltpu.VMEM((12, COL, C1), bf),
                pltpu.VMEM((12, MID_COL, C1), bf),
                pltpu.VMEM((10, MID_COL, 128), f32),
                pltpu.VMEM((len(BLOCKS), 2, 8 * OUT_COL, 128), f32),
                pltpu.SemaphoreType.REGULAR, dma, dma, pltpu.SemaphoreType.DMA((2,)), dma,
                dma, dma, dma, dma, dma, dma,
            ],
            compiler_params=pltpu.CompilerParams(collective_id=0, has_side_effects=True, vmem_limit_bytes=24 << 20),
        )(*(pltpu.with_memory_space_constraint(a, pltpu.HBM) for a in operands))
        return pl.pallas_call(
            kernel_two,
            name="conv_last",
            out_shape=jax.ShapeDtypeStruct((8, 16, 8, C2), f32),
            in_specs=[vmem] * 5,
            out_specs=hbm,
            scratch_shapes=[pltpu.VMEM((8, 16 - LAST, 8, C2), f32), pltpu.VMEM((2, 8 * OUT_COL, 128), f32), pltpu.SemaphoreType.DMA((2,))],
            compiler_params=pltpu.CompilerParams(vmem_limit_bytes=24 << 20),
        )(out_a, ys0, ys8, w2, operands[-1])

    return jax.shard_map(
        run_local,
        mesh=mesh,
        in_specs=(P("data", None, None, GROUP_AXES), P(None, None, GROUP_AXES, None), P(), P(), P()),
        out_specs=P("data", "model", "cols", None),
        check_vma=False,
    )
```
